16 devices in a mesh: replica: 2 (over y, z), model: 8 (over x, core).
Axes of the slice: x: 4, y: 2, z: 1, core: 2. Of those that a mesh axis runs over, the one named last changes fastest.
The devices are a block of a 4x4x8 slice.
Arguments:
- prompt: bfloat16 [64, 384, 3072], P('replica', 'model'), parts along dimension 0
- lengths: int32 [64], P('replica'), parts along dimension 0
- new_tok: bfloat16 [64, 3072], P('replica'), parts along dimension 0
- norm_attn: bfloat16 [1, 3072], replicated
- w_q: bfloat16 [1, 3072, 3072], P(None, None, 'model')
- w_k: bfloat16 [1, 3072, 1024], P(None, None, 'model')
- w_v: bfloat16 [1, 3072, 1024], P(None, None, 'model')
- w_o: bfloat16 [1, 3072, 3072], P(None, 'model')
- norm_mlp: bfloat16 [1, 3072], replicated
- w_gate: bfloat16 [1, 3072, 8192], P(None, None, 'model')
- w_up: bfloat16 [1, 3072, 8192], P(None, None, 'model')
- w_down: bfloat16 [1, 8192, 3072], P(None, 'model')
Outputs:
- output 1: bfloat16 [64, 3072], P('replica'), parts along dimension 0
- output 2: bfloat16 [64, 3072], P('replica'), parts along dimension 0
- output 3: bfloat16 [1, 64, 385, 8, 128], P(None, 'replica', None, 'model'), parts along dimension 1
- output 4: bfloat16 [1, 64, 385, 8, 128], P(None, 'replica', None, 'model'), parts along dimension 1
There are 2 independent parts. The reference program is written for one: setup_inputs(seed, part) draws one part's arguments, and reference() takes and returns one part's arrays. A program takes and returns all parts, laid end to end along the dimension named above; an argument that names none is the same for every part.
All inputs are finite; a program needn't handle non-finite values.
Results may differ from the reference program's by a relative error of at most 0.0109076.
Values are sent between devices in bfloat16 or wider.
A program may use at most 768 MiB of HBM per device.

```python
import jax
import jax.numpy as jnp
from jax import lax

BATCH_SIZE = 32
SEQ_LEN = 384
Q_BLOCK = 48
D_MODEL = 3072
NUM_HEADS = 24
KV_HEADS = 8
HEAD_DIM = 128
FF_DIM = 8192
N_LAYERS = 1

Q_WIDTH = NUM_HEADS * HEAD_DIM
KV_WIDTH = KV_HEADS * HEAD_DIM
GROUP_SIZE = NUM_HEADS // KV_HEADS
N_QBLOCKS = SEQ_LEN // Q_BLOCK
N_TOKENS = BATCH_SIZE * SEQ_LEN


def setup_inputs(seed: int = 0, part: int = 0) -> dict:
    part_keys = jax.random.split(jax.random.fold_in(jax.random.key(seed), part), 4)
    shared_keys = jax.random.split(jax.random.key(seed + 1), 9)
    qk_scale = (2.0 / D_MODEL) ** 0.5
    in_scale = D_MODEL ** -0.5

    def normal_bf16(rng_key, dims, scale_val):
        return (jax.random.normal(rng_key, dims, jnp.float32) * scale_val).astype(jnp.bfloat16)

    def gain_bf16(rng_key):
        return jax.random.uniform(rng_key, (N_LAYERS, D_MODEL), jnp.float32, 0.6, 1.4).astype(jnp.bfloat16)

    lengths = jax.random.randint(part_keys[1], (BATCH_SIZE,), SEQ_LEN // 2 + 1, SEQ_LEN + 1)
    full_row = jax.random.randint(part_keys[2], (), 0, BATCH_SIZE)
    lengths = jnp.where(jnp.arange(BATCH_SIZE) == full_row, SEQ_LEN, lengths).astype(jnp.int32)
    return {
        'prompt': normal_bf16(part_keys[0], (BATCH_SIZE, SEQ_LEN, D_MODEL), 1.0),
        'lengths': lengths,
        'new_tok': normal_bf16(part_keys[3], (BATCH_SIZE, D_MODEL), 1.0),
        'norm_attn': gain_bf16(shared_keys[0]),
        'w_q': normal_bf16(shared_keys[1], (N_LAYERS, D_MODEL, Q_WIDTH), qk_scale),
        'w_k': normal_bf16(shared_keys[2], (N_LAYERS, D_MODEL, KV_WIDTH), qk_scale),
        'w_v': normal_bf16(shared_keys[3], (N_LAYERS, D_MODEL, KV_WIDTH), in_scale),
        'w_o': normal_bf16(shared_keys[4], (N_LAYERS, Q_WIDTH, D_MODEL), Q_WIDTH ** -0.5),
        'norm_mlp': gain_bf16(shared_keys[5]),
        'w_gate': normal_bf16(shared_keys[6], (N_LAYERS, D_MODEL, FF_DIM), in_scale),
        'w_up': normal_bf16(shared_keys[7], (N_LAYERS, D_MODEL, FF_DIM), in_scale),
        'w_down': normal_bf16(shared_keys[8], (N_LAYERS, FF_DIM, D_MODEL), FF_DIM ** -0.5),
    }


def rms_norm(hidden, gain_vec):
    hid_f32 = hidden.astype(jnp.float32)
    inv_rms = lax.rsqrt(jnp.mean(hid_f32 * hid_f32, axis=-1, keepdims=True) + 1e-5)
    return (hid_f32 * inv_rms * gain_vec.astype(jnp.float32)).astype(jnp.bfloat16)


def rotary(heads_f32, positions):
    half_dim = HEAD_DIM // 2
    inv_freq = 10000.0 ** (-2.0 * jnp.arange(half_dim, dtype=jnp.float32) / HEAD_DIM)
    angles = positions.astype(jnp.float32)[..., None] * inv_freq
    cos_tab = jnp.cos(angles)[..., None, :]
    sin_tab = jnp.sin(angles)[..., None, :]
    lo_half = heads_f32[..., :half_dim]
    hi_half = heads_f32[..., half_dim:]
    return jnp.concatenate([lo_half * cos_tab - hi_half * sin_tab, hi_half * cos_tab + lo_half * sin_tab], axis=-1)


def prefill_attention(queries, key_rot, val_proj, lengths):
    q_blocks = jnp.moveaxis(queries.astype(jnp.float32).reshape(BATCH_SIZE, N_QBLOCKS, Q_BLOCK, KV_HEADS, GROUP_SIZE, HEAD_DIM), 1, 0)
    key_f32 = key_rot.astype(jnp.float32)
    val_f32 = val_proj.astype(jnp.float32)
    key_pos = jnp.arange(SEQ_LEN)
    key_valid = key_pos[None, :] < lengths[:, None]

    def one_block(block_args):
        q_blk, blk_idx = block_args
        q_pos = blk_idx * Q_BLOCK + jnp.arange(Q_BLOCK)
        scores = jnp.einsum('bqhgd,bkhd->bqhgk', q_blk, key_f32) * (HEAD_DIM ** -0.5)
        visible = (key_pos[None, None, :] <= q_pos[None, :, None]) & key_valid[:, None, :]
        scores = jnp.where(visible[:, :, None, None, :], scores, -1e30)
        attn_prob = jax.nn.softmax(scores, axis=-1)
        return jnp.einsum('bqhgk,bkhd->bqhgd', attn_prob, val_f32)

    blocks_out = lax.map(one_block, (q_blocks, jnp.arange(N_QBLOCKS)))
    return jnp.moveaxis(blocks_out, 0, 1).reshape(BATCH_SIZE, SEQ_LEN, Q_WIDTH).astype(jnp.bfloat16)


def decode_attention(q_new, key_cache, value_cache, lengths):
    q_f32 = q_new.astype(jnp.float32).reshape(BATCH_SIZE, KV_HEADS, GROUP_SIZE, HEAD_DIM)
    scores = jnp.einsum('bhgd,bkhd->bhgk', q_f32, key_cache.astype(jnp.float32)) * (HEAD_DIM ** -0.5)
    cache_pos = jnp.arange(SEQ_LEN + 1)
    visible = (cache_pos[None, :] < lengths[:, None]) | (cache_pos[None, :] == SEQ_LEN)
    scores = jnp.where(visible[:, None, None, :], scores, -1e30)
    attn_prob = jax.nn.softmax(scores, axis=-1)
    out_f32 = jnp.einsum('bhgk,bkhd->bhgd', attn_prob, value_cache.astype(jnp.float32))
    return out_f32.reshape(BATCH_SIZE, Q_WIDTH).astype(jnp.bfloat16)


def reference(prompt, lengths, new_tok, norm_attn, w_q, w_k, w_v, w_o, norm_mlp, w_gate, w_up, w_down):
    seq_pos = jnp.arange(SEQ_LEN)

    def layer_step(loop_state, layer_w):
        hidden, dec_hidden = loop_state
        g_attn, wq_l, wk_l, wv_l, wo_l, g_mlp, wg_l, wu_l, wd_l = layer_w
        normed = rms_norm(hidden, g_attn).reshape(N_TOKENS, D_MODEL)
        q_rot = rotary(jnp.dot(normed, wq_l, preferred_element_type=jnp.float32).reshape(BATCH_SIZE, SEQ_LEN, NUM_HEADS, HEAD_DIM), seq_pos).astype(jnp.bfloat16)
        k_rot = rotary(jnp.dot(normed, wk_l, preferred_element_type=jnp.float32).reshape(BATCH_SIZE, SEQ_LEN, KV_HEADS, HEAD_DIM), seq_pos).astype(jnp.bfloat16)
        v_proj = jnp.dot(normed, wv_l, preferred_element_type=jnp.float32).astype(jnp.bfloat16).reshape(BATCH_SIZE, SEQ_LEN, KV_HEADS, HEAD_DIM)
        attn_out = prefill_attention(q_rot, k_rot, v_proj, lengths).reshape(N_TOKENS, Q_WIDTH)
        hidden = (hidden.astype(jnp.float32) + jnp.dot(attn_out, wo_l, preferred_element_type=jnp.float32).reshape(BATCH_SIZE, SEQ_LEN, D_MODEL)).astype(jnp.bfloat16)
        normed = rms_norm(hidden, g_mlp).reshape(N_TOKENS, D_MODEL)
        mlp_mid = (jax.nn.silu(jnp.dot(normed, wg_l, preferred_element_type=jnp.float32)) * jnp.dot(normed, wu_l, preferred_element_type=jnp.float32)).astype(jnp.bfloat16)
        hidden = (hidden.astype(jnp.float32) + jnp.dot(mlp_mid, wd_l, preferred_element_type=jnp.float32).reshape(BATCH_SIZE, SEQ_LEN, D_MODEL)).astype(jnp.bfloat16)

        tok_norm = rms_norm(dec_hidden, g_attn)
        q_new = rotary(jnp.dot(tok_norm, wq_l, preferred_element_type=jnp.float32).reshape(BATCH_SIZE, NUM_HEADS, HEAD_DIM), lengths).astype(jnp.bfloat16)
        k_new = rotary(jnp.dot(tok_norm, wk_l, preferred_element_type=jnp.float32).reshape(BATCH_SIZE, KV_HEADS, HEAD_DIM), lengths).astype(jnp.bfloat16)
        v_new = jnp.dot(tok_norm, wv_l, preferred_element_type=jnp.float32).astype(jnp.bfloat16).reshape(BATCH_SIZE, KV_HEADS, HEAD_DIM)
        key_cache = jnp.concatenate([k_rot, k_new[:, None]], axis=1)
        value_cache = jnp.concatenate([v_proj, v_new[:, None]], axis=1)
        tok_attn = decode_attention(q_new, key_cache, value_cache, lengths)
        dec_hidden = (dec_hidden.astype(jnp.float32) + jnp.dot(tok_attn, wo_l, preferred_element_type=jnp.float32)).astype(jnp.bfloat16)
        tok_norm = rms_norm(dec_hidden, g_mlp)
        tok_mid = (jax.nn.silu(jnp.dot(tok_norm, wg_l, preferred_element_type=jnp.float32)) * jnp.dot(tok_norm, wu_l, preferred_element_type=jnp.float32)).astype(jnp.bfloat16)
        dec_hidden = (dec_hidden.astype(jnp.float32) + jnp.dot(tok_mid, wd_l, preferred_element_type=jnp.float32)).astype(jnp.bfloat16)
        return (hidden, dec_hidden), (key_cache, value_cache)

    (hidden, dec_hidden), (key_cache, value_cache) = lax.scan(layer_step, (prompt, new_tok), (norm_attn, w_q, w_k, w_v, w_o, norm_mlp, w_gate, w_up, w_down))
    last_sel = seq_pos[None, :] == (lengths - 1)[:, None]
    last_hidden = jnp.sum(jnp.where(last_sel[:, :, None], hidden.astype(jnp.float32), 0.0), axis=1).astype(jnp.bfloat16)
    return dec_hidden, last_hidden, key_cache, value_cache
```

```python
import jax
import jax.numpy as jnp
from jax import lax
from jax.sharding import PartitionSpec as P

HEAD_DIM = 128
NEG_BIG = -1e30


def rms_norm(hidden, gain_vec):
    hid_f32 = hidden.astype(jnp.float32)
    inv_rms = lax.rsqrt(jnp.mean(hid_f32 * hid_f32, axis=-1, keepdims=True) + 1e-5)
    return (hid_f32 * inv_rms * gain_vec.astype(jnp.float32)).astype(jnp.bfloat16)


def rotary(heads_f32, positions):
    half_dim = HEAD_DIM // 2
    inv_freq = 10000.0 ** (-2.0 * jnp.arange(half_dim, dtype=jnp.float32) / HEAD_DIM)
    angles = positions.astype(jnp.float32)[..., None] * inv_freq
    cos_tab = jnp.cos(angles)[..., None, :]
    sin_tab = jnp.sin(angles)[..., None, :]
    lo_half = heads_f32[..., :half_dim]
    hi_half = heads_f32[..., half_dim:]
    return jnp.concatenate([lo_half * cos_tab - hi_half * sin_tab, hi_half * cos_tab + lo_half * sin_tab], axis=-1)


def dot_f32(a, b):
    return jnp.dot(a, b, preferred_element_type=jnp.float32)


def solution(mesh):
    n_dev = mesh.shape['model']
    seq_spec = P('replica', 'model', None)
    col_spec = P(None, None, 'model')
    row_spec = P(None, 'model', None)
    gain_spec = P(None, None)
    tok_spec = P('replica', None)
    cache_spec = P(None, 'replica', None, 'model', None)
    in_specs = (seq_spec, P('replica'), tok_spec, gain_spec, col_spec, col_spec, col_spec, row_spec, gain_spec, col_spec, col_spec, row_spec)
    out_specs = (tok_spec, tok_spec, cache_spec, cache_spec)

    def per_device(prompt, lengths, new_tok, norm_attn, w_q, w_k, w_v, w_o, norm_mlp, w_gate, w_up, w_down):
        assert w_q.shape[0] == 1
        my_idx = lax.axis_index('model')
        n_batch, seq_loc, d_model = prompt.shape
        n_tok = n_batch * seq_loc
        seq_len = seq_loc * n_dev
        heads_loc = w_q.shape[2] // HEAD_DIM
        g_attn, wq, wk, wv, wo, g_mlp, wg, wu, wd = (a[0] for a in (norm_attn, w_q, w_k, w_v, w_o, norm_mlp, w_gate, w_up, w_down))
        seq_pos = my_idx * seq_loc + jnp.arange(seq_loc)
        wk_full = lax.all_gather(wk, 'model', axis=0, tiled=False)
        wv_full = lax.all_gather(wv, 'model', axis=0, tiled=False)
        normed = rms_norm(prompt, g_attn)
        k_all = jnp.einsum('bsd,jdh->jsbh', normed, wk_full, preferred_element_type=jnp.float32)
        v_all = jnp.einsum('bsd,jdh->jsbh', normed, wv_full, preferred_element_type=jnp.float32).astype(jnp.bfloat16)
        k_all = rotary(k_all, seq_pos).astype(jnp.bfloat16)
        key_mine = lax.all_to_all(k_all, 'model', 0, 0, tiled=False).reshape(seq_len, n_batch, HEAD_DIM)
        val_mine = lax.all_to_all(v_all, 'model', 0, 0, tiled=False).reshape(seq_len, n_batch, HEAD_DIM)
        last_sel = (seq_pos[None, :] == (lengths - 1)[:, None]).astype(jnp.bfloat16)
        last_row = jnp.einsum('bs,bsd->bd', last_sel, prompt, preferred_element_type=jnp.float32)
        last_row = lax.psum(last_row, 'model').astype(jnp.bfloat16)
        rows = jnp.concatenate([last_row, new_tok], axis=0)
        row_pos = jnp.concatenate([lengths - 1, lengths])
        row_norm = rms_norm(rows, g_attn)
        q_rows = rotary(dot_f32(row_norm, wq).reshape(2 * n_batch, heads_loc, HEAD_DIM), row_pos).astype(jnp.bfloat16)
        new_norm = row_norm[n_batch:]
        k_new = rotary(dot_f32(new_norm, wk)[:, None], lengths).astype(jnp.bfloat16)[:, 0]
        v_new = dot_f32(new_norm, wv).astype(jnp.bfloat16)
        key_cache = jnp.concatenate([key_mine, k_new[None]], axis=0)
        val_cache = jnp.concatenate([val_mine, v_new[None]], axis=0)
        q_grp = q_rows.reshape(2, n_batch, heads_loc, HEAD_DIM)
        scores = jnp.einsum('tbgd,kbd->btgk', q_grp, key_cache, preferred_element_type=jnp.float32) * (HEAD_DIM ** -0.5)
        slot = jnp.arange(seq_len + 1)
        old = slot[None, :] < lengths[:, None]
        visible = jnp.stack([old, old | (slot[None, :] == seq_len)], axis=1)
        scores = jnp.where(visible[:, :, None, :], scores, NEG_BIG)
        prob = jax.nn.softmax(scores, axis=-1).astype(jnp.bfloat16)
        attn = jnp.einsum('btgk,kbd->tbgd', prob, val_cache, preferred_element_type=jnp.float32)
        attn = attn.reshape(2 * n_batch, heads_loc * HEAD_DIM).astype(jnp.bfloat16)
        hidden = (rows.astype(jnp.float32) + lax.psum(dot_f32(attn, wo), 'model')).astype(jnp.bfloat16)
        mlp_in = rms_norm(hidden, g_mlp)
        mid = (jax.nn.silu(dot_f32(mlp_in, wg)) * dot_f32(mlp_in, wu)).astype(jnp.bfloat16)
        hidden = (hidden.astype(jnp.float32) + lax.psum(dot_f32(mid, wd), 'model')).astype(jnp.bfloat16)

        def as_cache(arr):
            return jnp.transpose(arr[None, :, :, None, :], (0, 2, 1, 3, 4))

        return hidden[n_batch:], hidden[:n_batch], as_cache(key_cache), as_cache(val_cache)

    return jax.shard_map(per_device, mesh=mesh, in_specs=in_specs, out_specs=out_specs, check_vma=False)
```

```python
import functools

import jax
import jax.numpy as jnp
from jax import lax
from jax.experimental import pallas as pl
from jax.experimental.pallas import tpu as pltpu
from jax.sharding import PartitionSpec as P

HEAD_DIM = 128
NEG_BIG = -1e30
CORES = 2
MESH_ID = pl.DeviceIdType.MESH
BF16 = jnp.bfloat16
F32 = jnp.float32


def dot_f32(a, b):
    return jnp.dot(a, b, preferred_element_type=F32)


def dot_bt(a, b):
    return lax.dot_general(a, b, (((1,), (1,)), ((), ())), preferred_element_type=F32)


def norm_rows(x_f32, gain_f32):
    inv_rms = lax.rsqrt(jnp.mean(x_f32 * x_f32, axis=-1, keepdims=True) + 1e-5)
    return x_f32 * inv_rms * gain_f32


def rotate(x_f32, cos_full, sin_signed):
    return x_f32 * cos_full + pltpu.roll(x_f32, HEAD_DIM // 2, 1) * sin_signed


def kernel(n_dev, n_batch, seq_loc, d_model, heads_loc, ff_loc,
           lens, prompt, new_tok, g_attn, g_mlp, cos_pos, sin_pos, cos_row, sin_row, len_row,
           wq, wk, wv, wo, wg, wu, wd,
           last_out, dec_out, kout, vout,
           xbuf, normed, wbuf, stage, kvrecv, relay, wq_v, wg_v, wu_v, res_k, res_v,
           last_f, xl_own, xl_sib, xl_sum, xl_recv, xl_half, xl_oth, rows_f, rows_n, q_s, knew, vnew,
           m_s, l_s, acc_s, part, d2d_in, rs_sum, rs_in, agbuf, x1_f, hid_n, part2, d2d_in2, rs_sum2, rs_in2, agbuf2,
           xsem, ldsem, w_send, w_recv, kv_send, kv_recv, rl_recv, xl_send, xl_rsem, out_sem, ar_send, ar_recv, ag_send, ag_recv):
    n_chip = n_dev // CORES
    n_tok = n_batch * seq_loc
    n_row = 2 * n_batch
    piece = n_row // n_dev
    half = d_model // 2
    me = lax.axis_index('model')
    c = me // CORES
    k = me % CORES
    o_core = 1 - k

    def dev(rel, kk):
        chip = lax.rem(c + rel, n_chip)
        return CORES * chip + (k if kk == 0 else o_core)

    RIGHT, OPP, LEFT = 1, 2, 3

    def slot(rel, kk):
        return rel * CORES + kk

    def rcopy(src, dst, ssem, rsem, target):
        return pltpu.make_async_remote_copy(src_ref=src, dst_ref=dst, send_sem=ssem, recv_sem=rsem,
                                            device_id={'model': target}, device_id_type=MESH_ID)

    own_w = slot(0, 0)
    ld_wk = pltpu.make_async_copy(wk, wbuf.at[own_w, :, pl.ds(0, HEAD_DIM)], ldsem.at[0])
    ld_wv = pltpu.make_async_copy(wv, wbuf.at[own_w, :, pl.ds(HEAD_DIM, HEAD_DIM)], ldsem.at[1])
    ld_wk.start()
    ld_wv.start()
    n_x = xbuf.shape[0]

    def x_copy(b, s):
        return pltpu.make_async_copy(prompt.at[b], xbuf.at[s], xsem.at[s])

    for b in range(n_x - 1):
        x_copy(b, b).start()

    barrier = pltpu.get_barrier_semaphore()
    for d in range(1, n_dev):
        pl.semaphore_signal(barrier, inc=1, device_id={'model': lax.rem(me + d, n_dev)}, device_id_type=MESH_ID)
    pl.semaphore_wait(barrier, n_dev - 1)

    def w_half(sl, h):
        return wbuf.at[sl, pl.ds(h * half, half), :]

    def w_copy(n, src_slot, dst_slot, h, target):
        return rcopy(w_half(src_slot, h), w_half(dst_slot, h), w_send.at[n], w_recv.at[dst_slot * 2 + h], target)

    ld_wk.wait()
    ld_wv.wait()
    sends = []
    to_r = [w_copy(0, own_w, slot(LEFT, 0), 0, dev(RIGHT, 0)), w_copy(1, own_w, slot(LEFT, 0), 1, dev(RIGHT, 0))]
    to_l = [w_copy(2, own_w, slot(RIGHT, 0), 1, dev(LEFT, 0)), w_copy(3, own_w, slot(RIGHT, 0), 0, dev(LEFT, 0))]
    to_s = [w_copy(4, own_w, slot(0, 1), 0, dev(0, 1)), w_copy(5, own_w, slot(0, 1), 1, dev(0, 1))]
    for cp in (to_r[0], to_l[0], to_r[1], to_l[1], to_s[0], to_s[1]):
        cp.start()
        sends.append(cp)
    fwd_r = w_copy(6, slot(LEFT, 0), slot(OPP, 0), 0, dev(RIGHT, 0))
    fwd_l = w_copy(7, slot(RIGHT, 0), slot(OPP, 0), 1, dev(LEFT, 0))
    sib_fwd = {}
    n = 8
    for rel in (LEFT, RIGHT, OPP):
        for h in range(2):
            sib_fwd[rel, h] = w_copy(n, slot(rel, 0), slot(rel, 1), h, dev(0, 1))
            n += 1

    ld_wq = pltpu.make_async_copy(wq, wq_v, ldsem.at[2])
    ld_wg = pltpu.make_async_copy(wg, wg_v, ldsem.at[3])
    ld_wu = pltpu.make_async_copy(wu, wu_v, ldsem.at[4])

    gain = g_attn[...].astype(F32)
    pos0 = me * seq_loc

    @pl.loop(0, n_batch)
    def _(b):
        s = lax.rem(b, n_x)

        @pl.when(b + n_x - 1 < n_batch)
        def _():
            x_copy(b + n_x - 1, lax.rem(b + n_x - 1, n_x)).start()

        x_copy(b, s).wait()
        x = xbuf[s].astype(F32)
        normed[pl.ds(pl.multiple_of(b * seq_loc, seq_loc), seq_loc), :] = norm_rows(x, gain).astype(BF16)
        here = (lax.broadcasted_iota(jnp.int32, (seq_loc, 1), 0) + pos0 == lens[b] - 1).astype(F32)
        last_f[pl.ds(b, 1), :] = jnp.sum(x * here, axis=0, keepdims=True)

    ld_wq.start()
    ld_wg.start()
    ld_wu.start()

    xl_own[...] = last_f[...].astype(BF16)
    xl_a = rcopy(xl_own, xl_sib, xl_send.at[0], xl_rsem.at[0], dev(0, 1))
    xl_a.start()

    def head(sl, dst):
        for_rows = 512

        @pl.loop(0, n_tok // for_rows)
        def _(m):
            r0 = pl.multiple_of(m * for_rows, for_rows)
            res = dot_f32(normed[pl.ds(r0, for_rows), :], wbuf[sl])
            res_k[pl.ds(r0, for_rows), :] = res[:, :HEAD_DIM]
            res_v[pl.ds(r0, for_rows), :] = res[:, HEAD_DIM:]

        @pl.loop(0, seq_loc, unroll=4)
        def _(s):
            rows = pl.ds(pl.multiple_of(s * n_batch, n_batch), n_batch)
            kt = res_k[pl.ds(s, n_batch, stride=seq_loc), :]
            dst[0, rows, :] = rotate(kt, cos_pos[pl.ds(s, 1), :], sin_pos[pl.ds(s, 1), :]).astype(BF16)
            dst[1, rows, :] = res_v[pl.ds(s, n_batch, stride=seq_loc), :].astype(BF16)

    def kv_slot_at_receiver(rel, kk):
        return slot((n_chip - rel) % n_chip, kk)

    def kv_copy(n, rel, kk):
        sl = kv_slot_at_receiver(rel, kk)
        return rcopy(stage.at[slot(rel, kk) - 1], kvrecv.at[sl], kv_send.at[n], kv_recv.at[sl], dev(rel, kk))

    head(own_w, kvrecv.at[own_w])

    def wait_w(rel, kk, h):
        w_copy(0, slot(rel, kk), slot(rel, kk), h, dev(0, 1)).wait_recv()

    wait_w(0, 1, 0)
    wait_w(0, 1, 1)
    head(slot(0, 1), stage.at[slot(0, 1) - 1])
    kv_sib = kv_copy(0, 0, 1)
    kv_sib.start()
    sends.append(kv_sib)

    hb = n_batch // CORES
    xl_a.wait_recv()
    my_rows = pl.ds(pl.multiple_of(k * hb, hb), hb)
    xl_sum[...] = xl_own[my_rows, :] + xl_sib[my_rows, :]
    xl_b = [rcopy(xl_sum, xl_recv.at[n_chip - 1 - rel], xl_send.at[rel], xl_rsem.at[n_chip - rel], dev(rel, 0)) for rel in (RIGHT, LEFT, OPP)]
    for cp in xl_b:
        cp.start()
    sends.append(xl_a)
    sends.extend(xl_b)

    wait_w(LEFT, 0, 0)
    fwd_r.start()
    sib_fwd[LEFT, 0].start()
    wait_w(RIGHT, 0, 1)
    fwd_l.start()
    sib_fwd[RIGHT, 1].start()
    sends += [fwd_r, fwd_l]
    wait_w(LEFT, 0, 1)
    sib_fwd[LEFT, 1].start()
    wait_w(RIGHT, 0, 0)
    sib_fwd[RIGHT, 0].start()
    n = 1
    kv_nb = {}
    for kk in range(2):
        for rel in (RIGHT, LEFT):
            if kk == 1:
                wait_w(rel, 1, 0)
                wait_w(rel, 1, 1)
            head(slot(rel, kk), stage.at[slot(rel, kk) - 1])
            kv_nb[rel, kk] = kv_copy(n, rel, kk)
            kv_nb[rel, kk].start()
            sends.append(kv_nb[rel, kk])
            n += 1
        if kk == 0:
            for cp in xl_b:
                cp.wait_recv()
            xl_half[...] = xl_sum[...] + xl_recv[0] + (xl_recv[1] + xl_recv[2])
            xl_c = rcopy(xl_half, xl_oth, xl_send.at[4], xl_rsem.at[4], dev(0, 1))
            xl_c.start()
            sends.append(xl_c)
    wait_w(OPP, 0, 0)
    sib_fwd[OPP, 0].start()
    wait_w(OPP, 0, 1)
    sib_fwd[OPP, 1].start()
    sends += list(sib_fwd.values())

    def relay_in(n, part_i, kk):
        return rcopy(stage.at[slot(OPP, kk) - 1, part_i], relay.at[part_i, kk], kv_send.at[n], rl_recv.at[part_i * 2 + kk],
                     dev(RIGHT if part_i == 0 else LEFT, 0))

    def relay_out(n, part_i, kk):
        sl = slot(OPP, kk)
        return rcopy(relay.at[part_i, kk], kvrecv.at[sl, part_i], kv_send.at[n], rl_recv.at[4 + part_i * 2 + kk],
                     dev(RIGHT if part_i == 0 else LEFT, kk))

    r_in = {}
    for kk in range(2):
        if kk == 1:
            wait_w(OPP, 1, 0)
            wait_w(OPP, 1, 1)
        head(slot(OPP, kk), stage.at[slot(OPP, kk) - 1])
        for p in range(2):
            r_in[p, kk] = relay_in(n, p, kk)
            r_in[p, kk].start()
            sends.append(r_in[p, kk])
            n += 1
    r_out = {(p, kk): relay_out(5 + 4 + p * 2 + kk, p, kk) for kk in range(2) for p in range(2)}

    wd_v = normed.at[pl.ds(0, ff_loc), :]
    wo_v = normed.at[pl.ds(ff_loc, heads_loc * HEAD_DIM), :]
    ld_wo = pltpu.make_async_copy(wo, wo_v, ldsem.at[0])
    ld_wd = pltpu.make_async_copy(wd, wd_v, ldsem.at[1])
    ld_wo.start()
    ld_wd.start()

    xl_c.wait_recv()
    oth_rows = pl.ds(pl.multiple_of(o_core * hb, hb), hb)
    rows_f[my_rows, :] = xl_half[...].astype(F32)
    rows_f[oth_rows, :] = xl_oth[...].astype(F32)
    rows_f[pl.ds(n_batch, n_batch), :] = new_tok[...].astype(F32)
    rows_n[...] = norm_rows(rows_f[...], gain).astype(BF16)
    ld_wq.wait()
    q_all = dot_f32(rows_n[...], wq_v[...])
    for g in range(heads_loc):
        q_g = rotate(q_all[:, g * HEAD_DIM:(g + 1) * HEAD_DIM], cos_row[...], sin_row[...])
        q_s[pl.ds(g * n_row, n_row), :] = q_g.astype(BF16)
    kv_new = dot_f32(rows_n[...], wbuf[own_w])
    new_rows = slice(n_batch, n_row)
    k_new = rotate(kv_new[new_rows, :HEAD_DIM], cos_row[pl.ds(n_batch, n_batch), :], sin_row[pl.ds(n_batch, n_batch), :])
    knew[...] = k_new.astype(BF16)
    vnew[...] = kv_new[new_rows, HEAD_DIM:].astype(BF16)
    tail_row = n_dev * n_tok
    outs = [pltpu.make_async_copy(knew, kout.at[pl.ds(tail_row, n_batch), :], out_sem.at[0]),
            pltpu.make_async_copy(vnew, vout.at[pl.ds(tail_row, n_batch), :], out_sem.at[1])]
    for cp in outs:
        cp.start()

    scale = HEAD_DIM ** -0.5
    n_q = heads_loc * n_row
    chunk = min(512, n_tok)
    m_s[...] = jnp.full(m_s.shape, NEG_BIG, F32)
    l_s[...] = jnp.zeros(l_s.shape, F32)
    acc_s[...] = jnp.zeros(acc_s.shape, F32)

    def update(sc, valid, v_blk):
        sc = jnp.where(valid, sc * scale, NEG_BIG)
        m_old = m_s[...]
        m_new = jnp.maximum(m_old, jnp.max(sc, axis=-1, keepdims=True))
        prob = jnp.where(valid, jnp.exp(sc - m_new), 0.0)
        alpha = jnp.exp(m_old - m_new)
        l_s[...] = l_s[...] * alpha + jnp.sum(prob, axis=-1, keepdims=True)
        acc_s[...] = acc_s[...] * alpha + dot_f32(prob.astype(BF16), v_blk)
        m_s[...] = m_new

    def attend(sl, src):
        @pl.loop(0, n_tok // chunk)
        def _(ch):
            rows = pl.ds(pl.multiple_of(ch * chunk, chunk), chunk)
            sc = dot_bt(q_s[...], kvrecv[sl, 0, rows, :])
            col = lax.broadcasted_iota(jnp.int32, (n_q, chunk), 1)
            row = lax.broadcasted_iota(jnp.int32, (n_q, chunk), 0)
            pos = src * seq_loc + ch * (chunk // n_batch) + col // n_batch
            valid = (col % n_batch == row % n_batch) & (pos < len_row[...])
            update(sc, valid, kvrecv[sl, 1, rows, :])

    def put_out(n, sl, src):
        rows = pl.ds(pl.multiple_of(src * n_tok, n_tok), n_tok)
        for i, ref in enumerate((kout, vout)):
            cp = pltpu.make_async_copy(kvrecv.at[sl, i], ref.at[rows, :], out_sem.at[2 + 2 * n + i])
            cp.start()
            outs.append(cp)

    col = lax.broadcasted_iota(jnp.int32, (n_q, n_batch), 1)
    row = lax.broadcasted_iota(jnp.int32, (n_q, n_batch), 0)
    is_new = (row // n_batch) % 2 == 1
    update(dot_bt(q_s[...], knew[...]), (col == row % n_batch) & is_new, vnew[...])
    put_out(0, own_w, me)
    attend(own_w, me)
    kv_sib.wait_recv()
    put_out(1, slot(0, 1), dev(0, 1))
    attend(slot(0, 1), dev(0, 1))
    n = 2
    for kk in range(2):
        for rel in (RIGHT, LEFT):
            src_rel = (n_chip - rel) % n_chip
            kv_nb[rel, kk].wait_recv()
            put_out(n, slot(src_rel, kk), dev(src_rel, kk))
            attend(slot(src_rel, kk), dev(src_rel, kk))
            n += 1
    for kk in range(2):
        for p in range(2):
            r_in[p, kk].wait_recv()
            r_out[p, kk].start()
            sends.append(r_out[p, kk])
    for kk in range(2):
        for p in range(2):
            r_out[p, kk].wait_recv()
        put_out(n, slot(OPP, kk), dev(OPP, kk))
        attend(slot(OPP, kk), dev(OPP, kk))
        n += 1
    o_all = (acc_s[...] / l_s[...]).astype(BF16)

    def sum_over_model(i, part_r, d2d_r, sum_r, in_r):
        cp = rcopy(part_r.at[o_core], d2d_r, ar_send.at[4 * i], ar_recv.at[4 * i], dev(0, 1))
        cp.start()
        cp.wait_recv()
        sends.append(cp)
        cps = []
        for rel in (OPP, RIGHT, LEFT):
            chip = lax.rem(c + rel, n_chip)
            sum_r[rel] = part_r[k, chip] + d2d_r[chip]
            cps.append(rcopy(sum_r.at[rel], in_r.at[n_chip - 1 - rel], ar_send.at[4 * i + rel], ar_recv.at[4 * i + n_chip - rel], dev(rel, 0)))
            cps[-1].start()
        total = part_r[k, c] + d2d_r[c]
        for cp in cps[1:] + cps[:1]:
            cp.wait_recv()
        sends.extend(cps)
        return total + in_r[0] + in_r[2] + in_r[1]

    def gather_rows(i, buf):
        cps = []
        for rel in (OPP, RIGHT, LEFT):
            cps.append(rcopy(buf.at[k, c], buf.at[k, c], ag_send.at[8 * i + rel], ag_recv.at[8 * i + n_chip - rel], dev(rel, 0)))
        cps.append(rcopy(buf.at[k, c], buf.at[k, c], ag_send.at[8 * i], ag_recv.at[8 * i], dev(0, 1)))
        for cp in cps:
            cp.start()
        fw = []
        for rel, cp in ((LEFT, cps[1]), (RIGHT, cps[2]), (OPP, cps[0])):
            cp.wait_recv()
            chip = lax.rem(c + rel, n_chip)
            f = rcopy(buf.at[k, chip], buf.at[k, chip], ag_send.at[8 * i + 4 + rel], ag_recv.at[8 * i + 4 + rel], dev(0, 1))
            f.start()
            fw.append(f)
        for cp in [cps[3]] + fw:
            cp.wait_recv()
        sends.extend(cps + fw)

    ld_wo.wait()
    o_rows = jnp.concatenate([o_all[g * n_row:(g + 1) * n_row] for g in range(heads_loc)], axis=1)
    for p in range(n_dev):
        r = slice(p * piece, (p + 1) * piece)
        if p == 0:
            o_out = dot_f32(o_rows, wo_v[...])
        part[p // n_chip, p % n_chip] = o_out[r]
    my_piece = pl.ds(pl.multiple_of((k * n_chip + c) * piece, piece), piece)
    att_sum = sum_over_model(0, part, d2d_in, rs_sum, rs_in)
    x1 = (rows_f[my_piece, :] + att_sum).astype(BF16).astype(F32)
    x1_f[...] = x1
    agbuf[k, c] = norm_rows(x1, g_mlp[...].astype(F32)).astype(BF16)
    gather_rows(0, agbuf)
    for p in range(0, n_dev, 2):
        two = [agbuf[i // n_chip, i % n_chip].astype(F32) for i in (p, p + 1)]
        hid_n[pl.ds(p * piece, 2 * piece), :] = jnp.concatenate(two, axis=0).astype(BF16)
    ld_wg.wait()
    ld_wu.wait()
    gate = dot_f32(hid_n[...], wg_v[...])
    up = dot_f32(hid_n[...], wu_v[...])
    mid = (gate * jax.nn.sigmoid(gate) * up).astype(BF16)
    ld_wd.wait()
    down = dot_f32(mid, wd_v[...])
    for p in range(n_dev):
        part2[p // n_chip, p % n_chip] = down[p * piece:(p + 1) * piece]
    mlp_sum = sum_over_model(1, part2, d2d_in2, rs_sum2, rs_in2)
    agbuf2[k, c] = (x1_f[...] + mlp_sum).astype(BF16)
    gather_rows(1, agbuf2)
    for p in range(0, n_dev, 2):
        two = jnp.concatenate([agbuf2[i // n_chip, i % n_chip].astype(F32) for i in (p, p + 1)], axis=0).astype(BF16)
        ref, r0 = (last_out, p * piece) if p * piece < n_batch else (dec_out, p * piece - n_batch)
        ref[pl.ds(r0, 2 * piece), :] = two
    for cp in sends:
        cp.wait_send()
    for cp in outs:
        cp.wait()


def solution(mesh):
    n_dev = mesh.shape['model']
    assert n_dev == 4 * CORES
    seq_spec = P('replica', 'model', None)
    col_spec = P(None, None, 'model')
    row_spec = P(None, 'model', None)
    gain_spec = P(None, None)
    tok_spec = P('replica', None)
    cache_spec = P(None, 'replica', None, 'model', None)
    in_specs = (seq_spec, P('replica'), tok_spec, gain_spec, col_spec, col_spec, col_spec, row_spec, gain_spec, col_spec, col_spec, row_spec)
    out_specs = (tok_spec, tok_spec, cache_spec, cache_spec)

    def tables(positions):
        half_dim = HEAD_DIM // 2
        inv_freq = 10000.0 ** (-2.0 * jnp.arange(half_dim, dtype=F32) / HEAD_DIM)
        angles = positions.astype(F32)[:, None] * inv_freq
        cos_tab, sin_tab = jnp.cos(angles), jnp.sin(angles)
        return jnp.concatenate([cos_tab, cos_tab], axis=1), jnp.concatenate([-sin_tab, sin_tab], axis=1)

    def per_device(prompt, lengths, new_tok, norm_attn, w_q, w_k, w_v, w_o, norm_mlp, w_gate, w_up, w_down):
        assert w_q.shape[0] == 1 and w_k.shape[2] == HEAD_DIM
        n_batch, seq_loc, d_model = prompt.shape
        n_tok = n_batch * seq_loc
        heads_loc = w_q.shape[2] // HEAD_DIM
        ff_loc = w_gate.shape[2]
        n_row = 2 * n_batch
        piece = n_row // n_dev
        n_chip = n_dev // CORES
        hb = n_batch // CORES
        n_q = heads_loc * n_row
        cos_pos, sin_pos = tables(lax.axis_index('model') * seq_loc + jnp.arange(seq_loc))
        cos_row, sin_row = tables(jnp.concatenate([lengths - 1, lengths]))
        len_row = jnp.tile(lengths, 2 * heads_loc)[:, None]
        vm = pl.BlockSpec(memory_space=pltpu.VMEM)
        hbm = pl.BlockSpec(memory_space=pl.ANY)
        V = pltpu.VMEM
        DMA = pltpu.SemaphoreType.DMA
        slab = (2, n_tok, HEAD_DIM)
        wide = (CORES, n_chip, piece, d_model)
        scratch = [
            V((4, seq_loc, d_model), BF16), V((n_tok, d_model), BF16), V((n_dev, d_model, 2 * HEAD_DIM), BF16),
            V((n_dev - 1,) + slab, BF16), V((n_dev,) + slab, BF16), V((2, 2, n_tok, HEAD_DIM), BF16),
            V((d_model, heads_loc * HEAD_DIM), BF16), V((d_model, ff_loc), BF16), V((d_model, ff_loc), BF16),
            V((n_tok, HEAD_DIM), F32), V((n_tok, HEAD_DIM), F32),
            V((n_batch, d_model), F32), V((n_batch, d_model), BF16), V((n_batch, d_model), BF16), V((hb, d_model), BF16),
            V((n_chip - 1, hb, d_model), BF16), V((hb, d_model), BF16), V((hb, d_model), BF16),
            V((n_row, d_model), F32), V((n_row, d_model), BF16), V((n_q, HEAD_DIM), BF16),
            V((n_batch, HEAD_DIM), BF16), V((n_batch, HEAD_DIM), BF16),
            V((n_q, 1), F32), V((n_q, 1), F32), V((n_q, HEAD_DIM), F32),
            V(wide, F32), V(wide[1:], F32), V(wide[1:], F32), V((n_chip - 1,) + wide[2:], F32), V(wide, BF16), V(wide[2:], F32),
            V((n_row, d_model), BF16),
            V(wide, F32), V(wide[1:], F32), V(wide[1:], F32), V((n_chip - 1,) + wide[2:], F32), V(wide, BF16),
            DMA((4,)), DMA((5,)), DMA((14,)), DMA((4 * n_dev,)), DMA((13,)), DMA((n_dev,)), DMA((8,)), DMA((5,)), DMA((5,)),
            DMA((2 + 2 * n_dev,)), DMA((8,)), DMA((8,)), DMA((16,)), DMA((16,)),
        ]
        cache = jax.ShapeDtypeStruct(((seq_loc * n_dev + 1) * n_batch, HEAD_DIM), BF16)
        tok = jax.ShapeDtypeStruct((n_batch, d_model), BF16)
        last, dec, kc, vc = pl.pallas_call(
            functools.partial(kernel, n_dev, n_batch, seq_loc, d_model, heads_loc, ff_loc),
            out_shape=[tok, tok, cache, cache],
            in_specs=[pl.BlockSpec(memory_space=pltpu.SMEM), hbm] + [vm] * 8 + [hbm] * 7,
            out_specs=[vm, vm, hbm, hbm],
            scratch_shapes=scratch,
            compiler_params=pltpu.CompilerParams(collective_id=0, has_side_effects=True, vmem_limit_bytes=67_043_328),
        )(lengths, prompt, new_tok, norm_attn, norm_mlp, cos_pos, sin_pos, cos_row, sin_row, len_row,
          w_q[0], w_k[0], w_v[0], w_o[0], w_gate[0], w_up[0], w_down[0])

        def as_cache(arr):
            return jnp.transpose(arr.reshape(1, seq_loc * n_dev + 1, 1, n_batch, HEAD_DIM), (0, 3, 1, 2, 4))

        return dec, last, as_cache(kc), as_cache(vc)

    return jax.shard_map(per_device, mesh=mesh, in_specs=in_specs, out_specs=out_specs, check_vma=False)
```

```python
import functools
import math

import jax
import jax.numpy as jnp
from jax import lax
from jax.experimental import pallas as pl
from jax.experimental.pallas import tpu as pltpu
from jax.sharding import PartitionSpec as P

HEAD_DIM = 128
NEG_BIG = -1e30
CORES = 2
N_BULK = 2
PLAN = (2, 1, 3, 1, 1)
MESH_ID = pl.DeviceIdType.MESH
BF16 = jnp.bfloat16
F32 = jnp.float32


def dot_f32(a, b):
    return jnp.dot(a, b, preferred_element_type=F32)


def dot_bt(a, b):
    return lax.dot_general(a, b, (((1,), (1,)), ((), ())), preferred_element_type=F32)


def norm_rows(x_f32, gain_f32):
    inv_rms = lax.rsqrt(jnp.mean(x_f32 * x_f32, axis=-1, keepdims=True) + 1e-5)
    return x_f32 * inv_rms * gain_f32


def rotate(x_f32, cos_full, sin_signed):
    return x_f32 * cos_full + pltpu.roll(x_f32, HEAD_DIM // 2, 1) * sin_signed


def kernel(n_dev, n_batch, seq_loc, d_model, heads_loc, ff_loc, n_bulk, plan,
           lens, prompt, new_tok, g_attn, g_mlp, wq, wk, wv, wo, wg, wu, wd,
           last_out, dec_out, kout, vout,
           xbuf, normed, wbuf, stage, kvrecv, wq_v, wg_v, wu_v, res_k, res_v,
           len_v, cos_pos, sin_pos, cos_row, sin_row,
           last_f, xl_own, xl_sib, xl_sum, xl_recv, xl_half, xl_oth, rows_f, rows_n, q_s, q_in, knew, vnew,
           m_s, l_s, acc_s, m_p, l_p, acc_p, msg, msg_in,
           part, d2d_in, rs_sum, rs_in, agbuf, x1_f, hid_n, part2, d2d_in2, rs_sum2, rs_in2, agbuf2,
           xsem, ldsem, w_send, w_recv, kv_send, kv_recv, bulk_send, bulk_recv, pt_send, pt_recv, xl_send, xl_rsem, out_sem,
           ar_send, ar_recv, ag_send, ag_recv):
    n_chip = n_dev // CORES
    n_tok = n_batch * seq_loc
    n_row = 2 * n_batch
    piece = n_row // n_dev
    half = d_model // 2
    me = lax.axis_index('model')
    c = me // CORES
    k = me % CORES
    o_core = 1 - k

    def dev(rel, kk):
        chip = lax.rem(c + rel, n_chip)
        return CORES * chip + (k if kk == 0 else o_core)

    RIGHT, OPP, LEFT = 1, 2, 3

    def slot(rel, kk):
        return rel * CORES + kk

    def rcopy(src, dst, ssem, rsem, target):
        return pltpu.make_async_remote_copy(src_ref=src, dst_ref=dst, send_sem=ssem, recv_sem=rsem,
                                            device_id={'model': target}, device_id_type=MESH_ID)

    own_w = slot(0, 0)
    ld_wk = pltpu.make_async_copy(wk, wbuf.at[own_w, :, pl.ds(0, HEAD_DIM)], ldsem.at[0])
    ld_wv = pltpu.make_async_copy(wv, wbuf.at[own_w, :, pl.ds(HEAD_DIM, HEAD_DIM)], ldsem.at[1])
    ld_wk.start()
    ld_wv.start()
    n_x = xbuf.shape[0]

    def x_copy(b, s):
        return pltpu.make_async_copy(prompt.at[b], xbuf.at[s], xsem.at[s])

    for b in range(n_x - 1):
        x_copy(b, b).start()

    barrier = pltpu.get_barrier_semaphore()
    for d in range(1, n_dev):
        pl.semaphore_signal(barrier, inc=1, device_id={'model': lax.rem(me + d, n_dev)}, device_id_type=MESH_ID)
    pl.semaphore_wait(barrier, n_dev - 1)

    def w_half(sl, h):
        return wbuf.at[sl, pl.ds(h * half, half), :]

    def w_copy(n, src_slot, dst_slot, h, target):
        return rcopy(w_half(src_slot, h), w_half(dst_slot, h), w_send.at[n], w_recv.at[dst_slot * 2 + h], target)

    ld_wk.wait()
    ld_wv.wait()
    sends = []

    def go(cp):
        cp.start()
        sends.append(cp)
        return cp

    to_r = [w_copy(0, own_w, slot(LEFT, 0), 0, dev(RIGHT, 0)), w_copy(1, own_w, slot(LEFT, 0), 1, dev(RIGHT, 0))]
    to_l = [w_copy(2, own_w, slot(RIGHT, 0), 1, dev(LEFT, 0)), w_copy(3, own_w, slot(RIGHT, 0), 0, dev(LEFT, 0))]
    to_s = [w_copy(4, own_w, slot(0, 1), 0, dev(0, 1)), w_copy(5, own_w, slot(0, 1), 1, dev(0, 1))]
    for cp in (to_r[0], to_l[0], to_s[0], to_s[1]):
        go(cp)
    fwd_r = w_copy(6, slot(LEFT, 0), slot(OPP, 0), 0, dev(RIGHT, 0))
    fwd_l = w_copy(7, slot(RIGHT, 0), slot(OPP, 0), 1, dev(LEFT, 0))
    sib_fwd = {}
    n = 8
    for rel in (LEFT, RIGHT, OPP):
        for h in range(2):
            sib_fwd[rel, h] = w_copy(n, slot(rel, 0), slot(rel, 1), h, dev(0, 1))
            n += 1

    ld_wq = pltpu.make_async_copy(wq, wq_v, ldsem.at[2])
    ld_wg = pltpu.make_async_copy(wg, wg_v, ldsem.at[3])
    ld_wu = pltpu.make_async_copy(wu, wu_v, ldsem.at[4])

    gain = g_attn[...].astype(F32)
    pos0 = me * seq_loc

    @pl.loop(0, n_batch)
    def _(b):
        s = lax.rem(b, n_x)

        @pl.when(b + n_x - 1 < n_batch)
        def _():
            x_copy(b + n_x - 1, lax.rem(b + n_x - 1, n_x)).start()

        x_copy(b, s).wait()
        x = xbuf[s].astype(F32)
        normed[pl.ds(pl.multiple_of(b * seq_loc, seq_loc), seq_loc), :] = norm_rows(x, gain).astype(BF16)
        here = (lax.broadcasted_iota(jnp.int32, (seq_loc, 1), 0) + pos0 == lens[b] - 1).astype(F32)
        last_f[pl.ds(b, 1), :] = jnp.sum(x * here, axis=0, keepdims=True)
        len_v[pl.ds(b, 1), :] = jnp.full((1, HEAD_DIM), lens[b], jnp.int32)

    ld_wq.start()
    ld_wg.start()
    ld_wu.start()

    xl_own[...] = last_f[...].astype(BF16)
    xl_a = go(rcopy(xl_own, xl_sib, xl_send.at[0], xl_rsem.at[0], dev(0, 1)))

    def table(cos_ref, sin_ref, rows, pos):
        lane = lax.broadcasted_iota(jnp.int32, pos.shape, 1)
        hd = HEAD_DIM // 2
        step = jnp.where(lane < hd, lane, lane - hd).astype(F32)
        angle = pos.astype(F32) * jnp.exp(step * (-2.0 * math.log(10000.0) / HEAD_DIM))
        cos_ref[rows, :] = jnp.cos(angle)
        sin_ref[rows, :] = jnp.where(lane < hd, -1.0, 1.0) * jnp.sin(angle)

    table(cos_pos, sin_pos, pl.ds(0, seq_loc), lax.broadcasted_iota(jnp.int32, (seq_loc, HEAD_DIM), 0) + pos0)
    table(cos_row, sin_row, pl.ds(0, n_batch), len_v[...] - 1)
    table(cos_row, sin_row, pl.ds(n_batch, n_batch), len_v[...])

    hb = n_batch // CORES
    xl_a.wait_recv()
    my_rows = pl.ds(pl.multiple_of(k * hb, hb), hb)
    oth_rows = pl.ds(pl.multiple_of(o_core * hb, hb), hb)
    xl_sum[...] = xl_own[my_rows, :] + xl_sib[my_rows, :]
    xl_b = [go(rcopy(xl_sum, xl_recv.at[n_chip - 1 - rel], xl_send.at[rel], xl_rsem.at[n_chip - rel], dev(rel, 0))) for rel in (RIGHT, LEFT, OPP)]
    go(to_r[1])
    go(to_l[1])

    def head(sl, dst):
        for_rows = 512

        @pl.loop(0, n_tok // for_rows)
        def _(m):
            r0 = pl.multiple_of(m * for_rows, for_rows)
            res = dot_f32(normed[pl.ds(r0, for_rows), :], wbuf[sl])
            res_k[pl.ds(r0, for_rows), :] = res[:, :HEAD_DIM]
            res_v[pl.ds(r0, for_rows), :] = res[:, HEAD_DIM:]

        @pl.loop(0, seq_loc, unroll=4)
        def _(s):
            rows = pl.ds(pl.multiple_of(s * n_batch, n_batch), n_batch)
            kt = res_k[pl.ds(s, n_batch, stride=seq_loc), :]
            dst[0, rows, :] = rotate(kt, cos_pos[pl.ds(s, 1), :], sin_pos[pl.ds(s, 1), :]).astype(BF16)
            dst[1, rows, :] = res_v[pl.ds(s, n_batch, stride=seq_loc), :].astype(BF16)

    def kv_copy(n, rel, kk):
        sl = slot((n_chip - rel) % n_chip, kk)
        return rcopy(stage.at[slot(rel, kk) - 1], kvrecv.at[sl], kv_send.at[n], kv_recv.at[sl], dev(rel, kk))

    def wait_w(rel, kk, h):
        w_copy(0, slot(rel, kk), slot(rel, kk), h, dev(0, 1)).wait_recv()

    head(own_w, kvrecv.at[own_w])
    wait_w(0, 1, 0)
    wait_w(0, 1, 1)
    head(slot(0, 1), stage.at[slot(0, 1) - 1])
    kv_sib = go(kv_copy(0, 0, 1))

    wait_w(LEFT, 0, 0)
    go(fwd_r)
    go(sib_fwd[LEFT, 0])
    wait_w(RIGHT, 0, 1)
    go(fwd_l)
    go(sib_fwd[RIGHT, 1])
    for cp in xl_b:
        cp.wait_recv()
    xl_half[...] = xl_sum[...] + xl_recv[0] + (xl_recv[1] + xl_recv[2])
    xl_c = go(rcopy(xl_half, xl_oth, xl_send.at[4], xl_rsem.at[4], dev(0, 1)))

    rows_f[my_rows, :] = xl_half[...].astype(F32)
    rows_f[pl.ds(n_batch, n_batch), :] = new_tok[...].astype(F32)
    ld_wq.wait()
    xl_c.wait_recv()
    rows_f[oth_rows, :] = xl_oth[...].astype(F32)
    rows_n[...] = norm_rows(rows_f[...], gain).astype(BF16)
    q_all = dot_f32(rows_n[...], wq_v[...])
    for g in range(heads_loc):
        q_g = rotate(q_all[:, g * HEAD_DIM:(g + 1) * HEAD_DIM], cos_row[...], sin_row[...])
        q_s[pl.ds(g * n_row, n_row), :] = q_g.astype(BF16)
    q_out = [go(rcopy(q_s, q_in.at[kk], pt_send.at[kk], pt_recv.at[kk], dev(OPP, kk))) for kk in range(2)]
    kv_new = dot_f32(rows_n[...], wbuf[own_w])
    new_rows = slice(n_batch, n_row)
    k_new = rotate(kv_new[new_rows, :HEAD_DIM], cos_row[pl.ds(n_batch, n_batch), :], sin_row[pl.ds(n_batch, n_batch), :])
    knew[...] = k_new.astype(BF16)
    vnew[...] = kv_new[new_rows, HEAD_DIM:].astype(BF16)
    tail_row = n_dev * n_tok
    outs = [pltpu.make_async_copy(knew, kout.at[pl.ds(tail_row, n_batch), :], out_sem.at[0]),
            pltpu.make_async_copy(vnew, vout.at[pl.ds(tail_row, n_batch), :], out_sem.at[1])]
    for cp in outs:
        cp.start()

    wait_w(LEFT, 0, 1)
    go(sib_fwd[LEFT, 1])
    wait_w(RIGHT, 0, 0)
    go(sib_fwd[RIGHT, 0])
    n = 1
    kv_nb = {}
    for kk in range(2):
        for rel in (RIGHT, LEFT):
            if kk == 1:
                wait_w(rel, 1, 0)
                wait_w(rel, 1, 1)
            head(slot(rel, kk), stage.at[slot(rel, kk) - 1])
            kv_nb[rel, kk] = go(kv_copy(n, rel, kk))
            n += 1
    wait_w(OPP, 0, 0)
    go(sib_fwd[OPP, 0])
    wait_w(OPP, 0, 1)
    go(sib_fwd[OPP, 1])

    scale = HEAD_DIM ** -0.5
    n_q = heads_loc * n_row
    chunk = min(512, n_tok)
    mine = (m_s, l_s, acc_s)

    def reset(state):
        state[0][...] = jnp.full(state[0].shape, NEG_BIG, F32)
        state[1][...] = jnp.zeros(state[1].shape, F32)
        state[2][...] = jnp.zeros(state[2].shape, F32)

    def update(state, sc, valid, v_blk):
        m_r, l_r, acc_r = state
        sc = jnp.where(valid, sc * scale, NEG_BIG)
        m_old = m_r[...]
        m_new = jnp.maximum(m_old, jnp.max(sc, axis=-1, keepdims=True))
        prob = jnp.where(valid, jnp.exp(sc - m_new), 0.0)
        alpha = jnp.exp(m_old - m_new)
        l_r[...] = l_r[...] * alpha + jnp.sum(prob, axis=-1, keepdims=True)
        acc_r[...] = acc_r[...] * alpha + dot_f32(prob.astype(BF16), v_blk)
        m_r[...] = m_new

    def attend(state, q_ref, kv_ref, src):
        @pl.loop(0, n_tok // chunk)
        def _(ch):
            rows = pl.ds(pl.multiple_of(ch * chunk, chunk), chunk)
            sc = dot_bt(q_ref[...], kv_ref[0, rows, :])
            col = lax.broadcasted_iota(jnp.int32, (n_q, chunk), 1)
            row = lax.broadcasted_iota(jnp.int32, (n_q, chunk), 0)
            pos = src * seq_loc + ch * (chunk // n_batch) + col // n_batch
            len_row = jnp.concatenate([len_v[:, :1]] * (n_q // n_batch), axis=0)
            valid = (col % n_batch == row % n_batch) & (pos < len_row)
            update(state, sc, valid, kv_ref[1, rows, :])

    lane_rows = [(i, min(HEAD_DIM, n_q - i)) for i in range(0, n_q, HEAD_DIM)]

    def on_diag(size):
        return lax.broadcasted_iota(jnp.int32, (size, HEAD_DIM), 0) == lax.broadcasted_iota(jnp.int32, (size, HEAD_DIM), 1)

    def put_column(ref, r0, column):
        for j, (i, size) in enumerate(lane_rows):
            ref[pl.ds(r0 + j, 1), :] = jnp.sum(jnp.where(on_diag(size), column[i:i + size], 0.0), axis=0, keepdims=True)

    def get_column(ref, r0):
        cols = [jnp.sum(jnp.where(on_diag(size), ref[pl.ds(r0 + j, 1), :], 0.0), axis=1, keepdims=True) for j, (i, size) in enumerate(lane_rows)]
        return jnp.concatenate(cols, axis=0)

    n_lr = len(lane_rows)
    pt_out = []
    for kk in range(2):
        if kk == 1:
            wait_w(OPP, 1, 0)
            wait_w(OPP, 1, 1)
        block = stage.at[slot(OPP, kk) - 1]
        head(slot(OPP, kk), block)
        q_out[kk].wait_recv()
        other = (m_p, l_p, acc_p)
        reset(other)
        attend(other, q_in.at[kk], block, me)
        msg[kk, pl.ds(0, n_q), :] = acc_p[...]
        put_column(msg.at[kk], n_q, m_p[...])
        put_column(msg.at[kk], n_q + n_lr, l_p[...])
        pt_out.append(go(rcopy(msg.at[kk], msg_in.at[kk], pt_send.at[2 + kk], pt_recv.at[2 + kk], dev(OPP, kk))))

    per = n_tok // n_bulk
    bulk = []
    for kk in range(2):
        for i in range(2):
            for j in range(n_bulk):
                rows = pl.ds(j * per, per)
                x = len(bulk)
                bulk.append(rcopy(stage.at[slot(OPP, kk) - 1, i, rows, :], kvrecv.at[slot(OPP, kk), i, rows, :], bulk_send.at[x], bulk_recv.at[x], dev(OPP, kk)))
    waiting = list(bulk)

    def send_bulk(count):
        for _ in range(count):
            if waiting:
                go(waiting.pop(0))

    send_bulk(plan[0])

    wd_v = normed.at[pl.ds(0, ff_loc), :]
    wo_v = normed.at[pl.ds(ff_loc, heads_loc * HEAD_DIM), :]
    ld_wo = pltpu.make_async_copy(wo, wo_v, ldsem.at[0])
    ld_wd = pltpu.make_async_copy(wd, wd_v, ldsem.at[1])
    ld_wo.start()
    ld_wd.start()

    def put_out(n, sl, src):
        rows = pl.ds(pl.multiple_of(src * n_tok, n_tok), n_tok)
        for i, ref in enumerate((kout, vout)):
            cp = pltpu.make_async_copy(kvrecv.at[sl, i], ref.at[rows, :], out_sem.at[2 + 2 * n + i])
            cp.start()
            outs.append(cp)

    reset(mine)
    col = lax.broadcasted_iota(jnp.int32, (n_q, n_batch), 1)
    row = lax.broadcasted_iota(jnp.int32, (n_q, n_batch), 0)
    is_new = (row // n_batch) % 2 == 1
    update(mine, dot_bt(q_s[...], knew[...]), (col == row % n_batch) & is_new, vnew[...])
    put_out(0, own_w, me)
    attend(mine, q_s, kvrecv.at[own_w], me)
    kv_sib.wait_recv()
    put_out(1, slot(0, 1), dev(0, 1))
    attend(mine, q_s, kvrecv.at[slot(0, 1)], dev(0, 1))
    n = 2
    for kk in range(2):
        for rel in (RIGHT, LEFT):
            src_rel = (n_chip - rel) % n_chip
            kv_nb[rel, kk].wait_recv()
            put_out(n, slot(src_rel, kk), dev(src_rel, kk))
            attend(mine, q_s, kvrecv.at[slot(src_rel, kk)], dev(src_rel, kk))
            n += 1
    for kk in range(2):
        pt_out[kk].wait_recv()
        m_o = get_column(msg_in.at[kk], n_q)
        l_o = get_column(msg_in.at[kk], n_q + n_lr)
        m_old = m_s[...]
        m_new = jnp.maximum(m_old, m_o)
        f_mine, f_oth = jnp.exp(m_old - m_new), jnp.exp(m_o - m_new)
        l_s[...] = l_s[...] * f_mine + l_o * f_oth
        acc_s[...] = acc_s[...] * f_mine + msg_in[kk, pl.ds(0, n_q), :] * f_oth
        m_s[...] = m_new
    o_all = (acc_s[...] / l_s[...]).astype(BF16)

    def sum_over_model(i, part_r, d2d_r, sum_r, in_r):
        cp = go(rcopy(part_r.at[o_core], d2d_r, ar_send.at[4 * i], ar_recv.at[4 * i], dev(0, 1)))
        cp.wait_recv()
        cps = []
        for rel in (OPP, RIGHT, LEFT):
            chip = lax.rem(c + rel, n_chip)
            sum_r[rel] = part_r[k, chip] + d2d_r[chip]
            cps.append(go(rcopy(sum_r.at[rel], in_r.at[n_chip - 1 - rel], ar_send.at[4 * i + rel], ar_recv.at[4 * i + n_chip - rel], dev(rel, 0))))
        send_bulk(plan[1 + 2 * i])
        total = part_r[k, c] + d2d_r[c]
        for cp in cps[1:] + cps[:1]:
            cp.wait_recv()
        return total + in_r[0] + in_r[2] + in_r[1]

    def gather_rows(i, buf):
        cps = []
        for rel in (OPP, RIGHT, LEFT):
            cps.append(go(rcopy(buf.at[k, c], buf.at[k, c], ag_send.at[8 * i + rel], ag_recv.at[8 * i + n_chip - rel], dev(rel, 0))))
        cps.append(go(rcopy(buf.at[k, c], buf.at[k, c], ag_send.at[8 * i], ag_recv.at[8 * i], dev(0, 1))))
        send_bulk(plan[2 + 2 * i])
        fw = []
        for rel, cp in ((LEFT, cps[1]), (RIGHT, cps[2]), (OPP, cps[0])):
            cp.wait_recv()
            chip = lax.rem(c + rel, n_chip)
            fw.append(go(rcopy(buf.at[k, chip], buf.at[k, chip], ag_send.at[8 * i + 4 + rel], ag_recv.at[8 * i + 4 + rel], dev(0, 1))))
        for cp in [cps[3]] + fw:
            cp.wait_recv()

    ld_wo.wait()
    o_rows = jnp.concatenate([o_all[g * n_row:(g + 1) * n_row] for g in range(heads_loc)], axis=1)
    o_out = dot_f32(o_rows, wo_v[...])
    for p in range(n_dev):
        part[p // n_chip, p % n_chip] = o_out[p * piece:(p + 1) * piece]
    my_piece = pl.ds(pl.multiple_of((k * n_chip + c) * piece, piece), piece)
    att_sum = sum_over_model(0, part, d2d_in, rs_sum, rs_in)
    x1 = (rows_f[my_piece, :] + att_sum).astype(BF16).astype(F32)
    x1_f[...] = x1
    agbuf[k, c] = norm_rows(x1, g_mlp[...].astype(F32)).astype(BF16)
    gather_rows(0, agbuf)
    for p in range(0, n_dev, 2):
        two = [agbuf[i // n_chip, i % n_chip].astype(F32) for i in (p, p + 1)]
        hid_n[pl.ds(p * piece, 2 * piece), :] = jnp.concatenate(two, axis=0).astype(BF16)
    ld_wg.wait()
    ld_wu.wait()
    gate = dot_f32(hid_n[...], wg_v[...])
    up = dot_f32(hid_n[...], wu_v[...])
    mid = (gate * jax.nn.sigmoid(gate) * up).astype(BF16)
    ld_wd.wait()
    down = dot_f32(mid, wd_v[...])
    for p in range(n_dev):
        part2[p // n_chip, p % n_chip] = down[p * piece:(p + 1) * piece]
    mlp_sum = sum_over_model(1, part2, d2d_in2, rs_sum2, rs_in2)
    agbuf2[k, c] = (x1_f[...] + mlp_sum).astype(BF16)
    gather_rows(1, agbuf2)
    send_bulk(len(waiting))
    for p in range(0, n_dev, 2):
        two = jnp.concatenate([agbuf2[i // n_chip, i % n_chip].astype(F32) for i in (p, p + 1)], axis=0).astype(BF16)
        ref, r0 = (last_out, p * piece) if p * piece < n_batch else (dec_out, p * piece - n_batch)
        ref[pl.ds(r0, 2 * piece), :] = two
    for kk in range(2):
        for cp in bulk[kk * 2 * n_bulk:(kk + 1) * 2 * n_bulk]:
            cp.wait_recv()
        put_out(n, slot(OPP, kk), dev(OPP, kk))
        n += 1
    for cp in sends:
        cp.wait_send()
    for cp in outs:
        cp.wait()


def write_kernel(n_part, last_in, dec_in, k_in, v_in, last_out, dec_out, k_out, v_out, tok_v, kv_v, in_sem, out_sem):
    rows = k_in.shape[0] // n_part
    pairs = [(last_in, last_out, tok_v.at[0]), (dec_in, dec_out, tok_v.at[1])]
    for p in range(n_part):
        for i, (src, dst) in enumerate(((k_in, k_out), (v_in, v_out))):
            r = pl.ds(p * rows, rows)
            pairs.append((src.at[r, :], dst.at[r, :], kv_v.at[i, r, :]))
    loads = [pltpu.make_async_copy(src, buf, in_sem.at[n]) for n, (src, dst, buf) in enumerate(pairs)]
    stores = [pltpu.make_async_copy(buf, dst, out_sem.at[n]) for n, (src, dst, buf) in enumerate(pairs)]
    for cp in loads:
        cp.start()
    for ld, st in zip(loads, stores):
        ld.wait()
        st.start()
    for cp in stores:
        cp.wait()


def solution(mesh):
    n_dev = mesh.shape['model']
    assert n_dev == 4 * CORES
    seq_spec = P('replica', 'model', None)
    col_spec = P(None, None, 'model')
    row_spec = P(None, 'model', None)
    gain_spec = P(None, None)
    tok_spec = P('replica', None)
    cache_spec = P(None, 'replica', None, 'model', None)
    in_specs = (seq_spec, P('replica'), tok_spec, gain_spec, col_spec, col_spec, col_spec, row_spec, gain_spec, col_spec, col_spec, row_spec)
    out_specs = (tok_spec, tok_spec, cache_spec, cache_spec)

    def per_device(prompt, lengths, new_tok, norm_attn, w_q, w_k, w_v, w_o, norm_mlp, w_gate, w_up, w_down):
        assert w_q.shape[0] == 1 and w_k.shape[2] == HEAD_DIM
        n_batch, seq_loc, d_model = prompt.shape
        n_tok = n_batch * seq_loc
        heads_loc = w_q.shape[2] // HEAD_DIM
        ff_loc = w_gate.shape[2]
        n_row = 2 * n_batch
        piece = n_row // n_dev
        n_chip = n_dev // CORES
        hb = n_batch // CORES
        n_q = heads_loc * n_row
        vm = pl.BlockSpec(memory_space=pltpu.VMEM)
        hbm = pl.BlockSpec(memory_space=pl.ANY)
        V = pltpu.VMEM
        DMA = pltpu.SemaphoreType.DMA
        slab = (2, n_tok, HEAD_DIM)
        wide = (CORES, n_chip, piece, d_model)
        n_lr = 2 * pl.cdiv(n_q, HEAD_DIM)
        state = [V((n_q, 1), F32), V((n_q, 1), F32), V((n_q, HEAD_DIM), F32)]
        note = V((2, pl.cdiv(n_q + n_lr, 8) * 8, HEAD_DIM), F32)
        scratch = [
            V((4, seq_loc, d_model), BF16), V((n_tok, d_model), BF16), V((n_dev, d_model, 2 * HEAD_DIM), BF16),
            V((n_dev - 1,) + slab, BF16), V((n_dev,) + slab, BF16),
            V((d_model, heads_loc * HEAD_DIM), BF16), V((d_model, ff_loc), BF16), V((d_model, ff_loc), BF16),
            V((n_tok, HEAD_DIM), F32), V((n_tok, HEAD_DIM), F32),
            V((n_batch, HEAD_DIM), jnp.int32), V((seq_loc, HEAD_DIM), F32), V((seq_loc, HEAD_DIM), F32), V((n_row, HEAD_DIM), F32), V((n_row, HEAD_DIM), F32),
            V((n_batch, d_model), F32), V((n_batch, d_model), BF16), V((n_batch, d_model), BF16), V((hb, d_model), BF16),
            V((n_chip - 1, hb, d_model), BF16), V((hb, d_model), BF16), V((hb, d_model), BF16),
            V((n_row, d_model), F32), V((n_row, d_model), BF16), V((n_q, HEAD_DIM), BF16), V((2, n_q, HEAD_DIM), BF16),
            V((n_batch, HEAD_DIM), BF16), V((n_batch, HEAD_DIM), BF16),
            *state, *state, note, note,
            V(wide, F32), V(wide[1:], F32), V(wide[1:], F32), V((n_chip - 1,) + wide[2:], F32), V(wide, BF16), V(wide[2:], F32),
            V((n_row, d_model), BF16),
            V(wide, F32), V(wide[1:], F32), V(wide[1:], F32), V((n_chip - 1,) + wide[2:], F32), V(wide, BF16),
            DMA((4,)), DMA((5,)), DMA((14,)), DMA((4 * n_dev,)), DMA((5,)), DMA((n_dev,)), DMA((4 * N_BULK,)), DMA((4 * N_BULK,)), DMA((4,)), DMA((4,)),
            DMA((5,)), DMA((5,)), DMA((2 + 2 * n_dev,)), DMA((8,)), DMA((8,)), DMA((16,)), DMA((16,)),
        ]
        cache_rows = (seq_loc * n_dev + 1) * n_batch
        cache = jax.ShapeDtypeStruct((cache_rows, HEAD_DIM), BF16)
        tok = jax.ShapeDtypeStruct((n_batch, d_model), BF16)
        made = pl.pallas_call(
            functools.partial(kernel, n_dev, n_batch, seq_loc, d_model, heads_loc, ff_loc, N_BULK, PLAN),
            out_shape=[tok, tok, cache, cache],
            in_specs=[pl.BlockSpec(memory_space=pltpu.SMEM), hbm] + [vm] * 3 + [hbm] * 7,
            out_specs=[vm, vm, hbm, hbm],
            scratch_shapes=scratch,
            compiler_params=pltpu.CompilerParams(collective_id=0, has_side_effects=True, vmem_limit_bytes=67_043_328),
        )(lengths, prompt, new_tok, norm_attn, norm_mlp, w_q[0], w_k[0], w_v[0], w_o[0], w_gate[0], w_up[0], w_down[0])
        n_part = next(p for p in range(4, cache_rows) if cache_rows // n_batch % p == 0)
        last, dec, kc, vc = pl.pallas_call(
            functools.partial(write_kernel, n_part),
            out_shape=[tok, tok, cache, cache],
            in_specs=[hbm] * 4,
            out_specs=[hbm] * 4,
            scratch_shapes=[V((2, n_batch, d_model), BF16), V((2, cache_rows, HEAD_DIM), BF16), DMA((2 + 2 * n_part,)), DMA((2 + 2 * n_part,))],
        )(*made)

        def as_cache(arr):
            return jnp.transpose(arr.reshape(1, seq_loc * n_dev + 1, 1, n_batch, HEAD_DIM), (0, 3, 1, 2, 4))

        return dec, last, as_cache(kc), as_cache(vc)

    return jax.shard_map(per_device, mesh=mesh, in_specs=in_specs, out_specs=out_specs, check_vma=False)
```

```python
import functools
import math

import jax
import jax.numpy as jnp
from jax import lax
from jax.experimental import pallas as pl
from jax.experimental.pallas import tpu as pltpu
from jax.sharding import PartitionSpec as P

HEAD_DIM = 128
NEG_BIG = -1e30
CORES = 2
N_BULK = 2
PLAN = (2, 1, 3, 1, 1)
MESH_ID = pl.DeviceIdType.MESH
BF16 = jnp.bfloat16
F32 = jnp.float32


def dot_f32(a, b):
    return jnp.dot(a, b, preferred_element_type=F32)


def dot_bt(a, b):
    return lax.dot_general(a, b, (((1,), (1,)), ((), ())), preferred_element_type=F32)


def norm_rows(x_f32, gain_f32):
    inv_rms = lax.rsqrt(jnp.mean(x_f32 * x_f32, axis=-1, keepdims=True) + 1e-5)
    return x_f32 * inv_rms * gain_f32


def rotate(x_f32, cos_full, sin_signed):
    return x_f32 * cos_full + pltpu.roll(x_f32, HEAD_DIM // 2, 1) * sin_signed


def kernel(n_dev, n_batch, seq_loc, d_model, heads_loc, ff_loc, n_bulk, plan,
           lens, prompt, new_tok, g_attn, g_mlp, wq, wk, wv, wo, wg, wu, wd,
           last_out, dec_out, kout, vout,
           xbuf, normed, wbuf, stage, kvrecv, wq_v, wg_v, wu_v, res_k, res_v,
           len_v, cos_pos, sin_pos, cos_row, sin_row,
           last_f, xl_own, xl_sib, xl_sum, xl_recv, xl_half, xl_oth, rows_f, rows_n, q_s, q_in, knew, vnew,
           m_s, l_s, acc_s, m_p, l_p, acc_p, msg, msg_in,
           part, d2d_in, rs_sum, rs_in, agbuf, x1_f, hid_n, part2, d2d_in2, rs_sum2, rs_in2, agbuf2,
           xsem, ldsem, w_send, w_recv, kv_send, kv_recv, bulk_send, bulk_recv, pt_send, pt_recv, xl_send, xl_rsem, out_sem,
           ar_send, ar_recv, ag_send, ag_recv):
    n_chip = n_dev // CORES
    n_tok = n_batch * seq_loc
    n_row = 2 * n_batch
    piece = n_row // n_dev
    quarter = d_model // 4
    me = lax.axis_index('model')
    c = me // CORES
    k = me % CORES
    o_core = 1 - k
    replica = lax.axis_index('replica')
    odd = lax.rem(replica, 2)
    partner = {'replica': replica + 1 - 2 * odd}

    def dev(rel, kk):
        chip = lax.rem(c + rel, n_chip)
        return CORES * chip + (k if kk == 0 else o_core)

    RIGHT, OPP, LEFT = 1, 2, 3

    def slot(rel, kk):
        return rel * CORES + kk

    def rcopy(src, dst, ssem, rsem, target):
        target = target if isinstance(target, dict) else {'model': target}
        return pltpu.make_async_remote_copy(src_ref=src, dst_ref=dst, send_sem=ssem, recv_sem=rsem,
                                            device_id=target, device_id_type=MESH_ID)

    own_w = slot(0, 0)
    ld_wk = pltpu.make_async_copy(wk, wbuf.at[own_w, :, pl.ds(0, HEAD_DIM)], ldsem.at[0])
    ld_wv = pltpu.make_async_copy(wv, wbuf.at[own_w, :, pl.ds(HEAD_DIM, HEAD_DIM)], ldsem.at[1])
    ld_wk.start()
    ld_wv.start()
    n_x = xbuf.shape[0]

    def x_copy(b, s):
        return pltpu.make_async_copy(prompt.at[b], xbuf.at[s], xsem.at[s])

    for b in range(n_x - 1):
        x_copy(b, b).start()

    barrier = pltpu.get_barrier_semaphore()
    for d in range(1, n_dev):
        pl.semaphore_signal(barrier, inc=1, device_id={'model': lax.rem(me + d, n_dev)}, device_id_type=MESH_ID)
    pl.semaphore_signal(barrier, inc=1, device_id=partner, device_id_type=MESH_ID)
    pl.semaphore_wait(barrier, n_dev)

    order = [i + odd * (3 - 2 * i) for i in range(4)]

    def w_part(sl, i):
        return wbuf.at[sl, pl.ds(pl.multiple_of(order[i] * quarter, quarter), quarter), :]

    def w_copy(n, src_slot, dst_slot, i, target, i_there=None):
        sem = w_recv.at[dst_slot * 4 + (i if i_there is None else i_there)]
        return rcopy(w_part(src_slot, i), w_part(dst_slot, i), w_send.at[n], sem, target)

    ld_wk.wait()
    ld_wv.wait()
    sends = []

    def go(cp):
        cp.start()
        sends.append(cp)
        return cp

    to_r = [w_copy(i, own_w, slot(LEFT, 0), i, dev(RIGHT, 0)) for i in range(3)]
    to_l = [w_copy(3 + i, own_w, slot(RIGHT, 0), i, dev(LEFT, 0)) for i in range(3)]
    to_s = rcopy(wbuf.at[own_w], wbuf.at[slot(0, 1)], w_send.at[6], w_recv.at[slot(0, 1) * 4], dev(0, 1))
    for cp in (to_r[0], to_l[0], to_r[1], to_l[1], to_s):
        go(cp)
    fwd_r = w_copy(7, slot(LEFT, 0), slot(OPP, 0), 0, dev(RIGHT, 0))
    fwd_l = w_copy(8, slot(RIGHT, 0), slot(OPP, 0), 1, dev(LEFT, 0))
    to_p = {(rel, i): w_copy(9 + n, slot(rel, 0), slot(rel, 0), i, partner, 3 - i)
            for n, (rel, i) in enumerate(((LEFT, 0), (RIGHT, 0), (OPP, 0), (OPP, 1)))}
    sib_fwd = {(rel, i): w_copy(13 + 4 * n + i, slot(rel, 0), slot(rel, 1), i, dev(0, 1))
               for n, rel in enumerate((LEFT, RIGHT, OPP)) for i in range(4)}

    ld_wq = pltpu.make_async_copy(wq, wq_v, ldsem.at[2])
    ld_wg = pltpu.make_async_copy(wg, wg_v, ldsem.at[3])
    ld_wu = pltpu.make_async_copy(wu, wu_v, ldsem.at[4])

    gain = g_attn[...].astype(F32)
    pos0 = me * seq_loc

    @pl.loop(0, n_batch)
    def _(b):
        s = lax.rem(b, n_x)

        @pl.when(b + n_x - 1 < n_batch)
        def _():
            x_copy(b + n_x - 1, lax.rem(b + n_x - 1, n_x)).start()

        x_copy(b, s).wait()
        x = xbuf[s].astype(F32)
        normed[pl.ds(pl.multiple_of(b * seq_loc, seq_loc), seq_loc), :] = norm_rows(x, gain).astype(BF16)
        here = (lax.broadcasted_iota(jnp.int32, (seq_loc, 1), 0) + pos0 == lens[b] - 1).astype(F32)
        last_f[pl.ds(b, 1), :] = jnp.sum(x * here, axis=0, keepdims=True)
        len_v[pl.ds(b, 1), :] = jnp.full((1, HEAD_DIM), lens[b], jnp.int32)

    ld_wq.start()
    ld_wg.start()
    ld_wu.start()

    xl_own[...] = last_f[...].astype(BF16)
    xl_a = go(rcopy(xl_own, xl_sib, xl_send.at[0], xl_rsem.at[0], dev(0, 1)))

    def table(cos_ref, sin_ref, rows, pos):
        lane = lax.broadcasted_iota(jnp.int32, pos.shape, 1)
        hd = HEAD_DIM // 2
        step = jnp.where(lane < hd, lane, lane - hd).astype(F32)
        angle = pos.astype(F32) * jnp.exp(step * (-2.0 * math.log(10000.0) / HEAD_DIM))
        cos_ref[rows, :] = jnp.cos(angle)
        sin_ref[rows, :] = jnp.where(lane < hd, -1.0, 1.0) * jnp.sin(angle)

    table(cos_pos, sin_pos, pl.ds(0, seq_loc), lax.broadcasted_iota(jnp.int32, (seq_loc, HEAD_DIM), 0) + pos0)
    table(cos_row, sin_row, pl.ds(0, n_batch), len_v[...] - 1)
    table(cos_row, sin_row, pl.ds(n_batch, n_batch), len_v[...])

    hb = n_batch // CORES
    xl_a.wait_recv()
    my_rows = pl.ds(pl.multiple_of(k * hb, hb), hb)
    oth_rows = pl.ds(pl.multiple_of(o_core * hb, hb), hb)
    xl_sum[...] = xl_own[my_rows, :] + xl_sib[my_rows, :]
    xl_b = [go(rcopy(xl_sum, xl_recv.at[n_chip - 1 - rel], xl_send.at[rel], xl_rsem.at[n_chip - rel], dev(rel, 0))) for rel in (RIGHT, LEFT, OPP)]
    go(to_r[2])
    go(to_l[2])

    def head(sl, dst):
        for_rows = 512

        @pl.loop(0, n_tok // for_rows)
        def _(m):
            r0 = pl.multiple_of(m * for_rows, for_rows)
            res = dot_f32(normed[pl.ds(r0, for_rows), :], wbuf[sl])
            res_k[pl.ds(r0, for_rows), :] = res[:, :HEAD_DIM]
            res_v[pl.ds(r0, for_rows), :] = res[:, HEAD_DIM:]

        @pl.loop(0, seq_loc, unroll=4)
        def _(s):
            rows = pl.ds(pl.multiple_of(s * n_batch, n_batch), n_batch)
            kt = res_k[pl.ds(s, n_batch, stride=seq_loc), :]
            dst[0, rows, :] = rotate(kt, cos_pos[pl.ds(s, 1), :], sin_pos[pl.ds(s, 1), :]).astype(BF16)
            dst[1, rows, :] = res_v[pl.ds(s, n_batch, stride=seq_loc), :].astype(BF16)

    def kv_copy(n, rel, kk):
        sl = slot((n_chip - rel) % n_chip, kk)
        return rcopy(stage.at[slot(rel, kk) - 1], kvrecv.at[sl], kv_send.at[n], kv_recv.at[sl], dev(rel, kk))

    def wait_w(rel, kk, i):
        w_copy(0, slot(rel, kk), slot(rel, kk), i, dev(0, 1)).wait_recv()

    for rel in (LEFT, RIGHT):
        wait_w(rel, 0, 0)
        go(to_p[rel, 0])
        go(sib_fwd[rel, 0])
        if rel == LEFT:
            go(fwd_r)
    head(own_w, kvrecv.at[own_w])
    for rel in (RIGHT, LEFT):
        wait_w(rel, 0, 1)
        if rel == RIGHT:
            go(fwd_l)
        go(sib_fwd[rel, 1])
    to_s.wait_recv()
    head(slot(0, 1), stage.at[slot(0, 1) - 1])
    kv_sib = go(kv_copy(0, 0, 1))

    for cp in xl_b:
        cp.wait_recv()
    xl_half[...] = xl_sum[...] + xl_recv[0] + (xl_recv[1] + xl_recv[2])
    xl_c = go(rcopy(xl_half, xl_oth, xl_send.at[4], xl_rsem.at[4], dev(0, 1)))

    rows_f[my_rows, :] = xl_half[...].astype(F32)
    rows_f[pl.ds(n_batch, n_batch), :] = new_tok[...].astype(F32)
    ld_wq.wait()
    xl_c.wait_recv()
    rows_f[oth_rows, :] = xl_oth[...].astype(F32)
    rows_n[...] = norm_rows(rows_f[...], gain).astype(BF16)
    q_all = dot_f32(rows_n[...], wq_v[...])
    for g in range(heads_loc):
        q_g = rotate(q_all[:, g * HEAD_DIM:(g + 1) * HEAD_DIM], cos_row[...], sin_row[...])
        q_s[pl.ds(g * n_row, n_row), :] = q_g.astype(BF16)
    q_out = [go(rcopy(q_s, q_in.at[kk], pt_send.at[kk], pt_recv.at[kk], dev(OPP, kk))) for kk in range(2)]
    kv_new = dot_f32(rows_n[...], wbuf[own_w])
    new_rows = slice(n_batch, n_row)
    k_new = rotate(kv_new[new_rows, :HEAD_DIM], cos_row[pl.ds(n_batch, n_batch), :], sin_row[pl.ds(n_batch, n_batch), :])
    knew[...] = k_new.astype(BF16)
    vnew[...] = kv_new[new_rows, HEAD_DIM:].astype(BF16)
    tail_row = n_dev * n_tok
    outs = [pltpu.make_async_copy(knew, kout.at[pl.ds(tail_row, n_batch), :], out_sem.at[0]),
            pltpu.make_async_copy(vnew, vout.at[pl.ds(tail_row, n_batch), :], out_sem.at[1])]
    for cp in outs:
        cp.start()

    for rel in (LEFT, RIGHT):
        for i in (3, 2):
            wait_w(rel, 0, i)
            go(sib_fwd[rel, i])
    n = 1
    kv_nb = {}
    for kk in range(2):
        for rel in (RIGHT, LEFT):
            if kk == 1:
                for i in range(4):
                    wait_w(rel, 1, i)
            head(slot(rel, kk), stage.at[slot(rel, kk) - 1])
            kv_nb[rel, kk] = go(kv_copy(n, rel, kk))
            n += 1
        if kk == 0:
            for i in range(2):
                wait_w(OPP, 0, i)
                go(to_p[OPP, i])
                go(sib_fwd[OPP, i])

    scale = HEAD_DIM ** -0.5
    n_q = heads_loc * n_row
    chunk = min(512, n_tok)
    mine = (m_s, l_s, acc_s)

    def reset(state):
        state[0][...] = jnp.full(state[0].shape, NEG_BIG, F32)
        state[1][...] = jnp.zeros(state[1].shape, F32)
        state[2][...] = jnp.zeros(state[2].shape, F32)

    def update(state, sc, valid, v_blk):
        m_r, l_r, acc_r = state
        sc = jnp.where(valid, sc * scale, NEG_BIG)
        m_old = m_r[...]
        m_new = jnp.maximum(m_old, jnp.max(sc, axis=-1, keepdims=True))
        prob = jnp.where(valid, jnp.exp(sc - m_new), 0.0)
        alpha = jnp.exp(m_old - m_new)
        l_r[...] = l_r[...] * alpha + jnp.sum(prob, axis=-1, keepdims=True)
        acc_r[...] = acc_r[...] * alpha + dot_f32(prob.astype(BF16), v_blk)
        m_r[...] = m_new

    def attend(state, q_ref, kv_ref, src):
        @pl.loop(0, n_tok // chunk)
        def _(ch):
            rows = pl.ds(pl.multiple_of(ch * chunk, chunk), chunk)
            sc = dot_bt(q_ref[...], kv_ref[0, rows, :])
            col = lax.broadcasted_iota(jnp.int32, (n_q, chunk), 1)
            row = lax.broadcasted_iota(jnp.int32, (n_q, chunk), 0)
            pos = src * seq_loc + ch * (chunk // n_batch) + col // n_batch
            len_row = jnp.concatenate([len_v[:, :1]] * (n_q // n_batch), axis=0)
            valid = (col % n_batch == row % n_batch) & (pos < len_row)
            update(state, sc, valid, kv_ref[1, rows, :])

    lane_rows = [(i, min(HEAD_DIM, n_q - i)) for i in range(0, n_q, HEAD_DIM)]

    def on_diag(size):
        return lax.broadcasted_iota(jnp.int32, (size, HEAD_DIM), 0) == lax.broadcasted_iota(jnp.int32, (size, HEAD_DIM), 1)

    def put_column(ref, r0, column):
        for j, (i, size) in enumerate(lane_rows):
            ref[pl.ds(r0 + j, 1), :] = jnp.sum(jnp.where(on_diag(size), column[i:i + size], 0.0), axis=0, keepdims=True)

    def get_column(ref, r0):
        cols = [jnp.sum(jnp.where(on_diag(size), ref[pl.ds(r0 + j, 1), :], 0.0), axis=1, keepdims=True) for j, (i, size) in enumerate(lane_rows)]
        return jnp.concatenate(cols, axis=0)

    def put_out(n, sl, src):
        rows = pl.ds(pl.multiple_of(src * n_tok, n_tok), n_tok)
        for i, ref in enumerate((kout, vout)):
            cp = pltpu.make_async_copy(kvrecv.at[sl, i], ref.at[rows, :], out_sem.at[2 + 2 * n + i])
            cp.start()
            outs.append(cp)

    reset(mine)
    col = lax.broadcasted_iota(jnp.int32, (n_q, n_batch), 1)
    row = lax.broadcasted_iota(jnp.int32, (n_q, n_batch), 0)
    is_new = (row // n_batch) % 2 == 1
    update(mine, dot_bt(q_s[...], knew[...]), (col == row % n_batch) & is_new, vnew[...])
    put_out(0, own_w, me)
    attend(mine, q_s, kvrecv.at[own_w], me)
    kv_sib.wait_recv()
    put_out(1, slot(0, 1), dev(0, 1))
    attend(mine, q_s, kvrecv.at[slot(0, 1)], dev(0, 1))

    n_lr = len(lane_rows)
    pt_out = []
    for i in (3, 2):
        wait_w(OPP, 0, i)
        go(sib_fwd[OPP, i])
    for kk in range(2):
        if kk == 1:
            for i in range(4):
                wait_w(OPP, 1, i)
        block = stage.at[slot(OPP, kk) - 1]
        head(slot(OPP, kk), block)
        q_out[kk].wait_recv()
        other = (m_p, l_p, acc_p)
        reset(other)
        attend(other, q_in.at[kk], block, me)
        msg[kk, pl.ds(0, n_q), :] = acc_p[...]
        put_column(msg.at[kk], n_q, m_p[...])
        put_column(msg.at[kk], n_q + n_lr, l_p[...])
        pt_out.append(go(rcopy(msg.at[kk], msg_in.at[kk], pt_send.at[2 + kk], pt_recv.at[2 + kk], dev(OPP, kk))))

    per = n_tok // n_bulk
    bulk = []
    for kk in range(2):
        for i in range(2):
            for j in range(n_bulk):
                rows = pl.ds(j * per, per)
                x = len(bulk)
                bulk.append(rcopy(stage.at[slot(OPP, kk) - 1, i, rows, :], kvrecv.at[slot(OPP, kk), i, rows, :], bulk_send.at[x], bulk_recv.at[x], dev(OPP, kk)))
    waiting = list(bulk)

    def send_bulk(count):
        for _ in range(count):
            if waiting:
                go(waiting.pop(0))

    send_bulk(plan[0])

    wd_v = normed.at[pl.ds(0, ff_loc), :]
    wo_v = normed.at[pl.ds(ff_loc, heads_loc * HEAD_DIM), :]
    ld_wo = pltpu.make_async_copy(wo, wo_v, ldsem.at[0])
    ld_wd = pltpu.make_async_copy(wd, wd_v, ldsem.at[1])
    ld_wo.start()
    ld_wd.start()

    n = 2
    for kk in range(2):
        for rel in (RIGHT, LEFT):
            src_rel = (n_chip - rel) % n_chip
            kv_nb[rel, kk].wait_recv()
            put_out(n, slot(src_rel, kk), dev(src_rel, kk))
            attend(mine, q_s, kvrecv.at[slot(src_rel, kk)], dev(src_rel, kk))
            n += 1
    for kk in range(2):
        pt_out[kk].wait_recv()
        m_o = get_column(msg_in.at[kk], n_q)
        l_o = get_column(msg_in.at[kk], n_q + n_lr)
        m_old = m_s[...]
        m_new = jnp.maximum(m_old, m_o)
        f_mine, f_oth = jnp.exp(m_old - m_new), jnp.exp(m_o - m_new)
        l_s[...] = l_s[...] * f_mine + l_o * f_oth
        acc_s[...] = acc_s[...] * f_mine + msg_in[kk, pl.ds(0, n_q), :] * f_oth
        m_s[...] = m_new
    o_all = (acc_s[...] / l_s[...]).astype(BF16)

    def sum_over_model(i, part_r, d2d_r, sum_r, in_r):
        cp = go(rcopy(part_r.at[o_core], d2d_r, ar_send.at[4 * i], ar_recv.at[4 * i], dev(0, 1)))
        cp.wait_recv()
        cps = []
        for rel in (OPP, RIGHT, LEFT):
            chip = lax.rem(c + rel, n_chip)
            sum_r[rel] = part_r[k, chip] + d2d_r[chip]
            cps.append(go(rcopy(sum_r.at[rel], in_r.at[n_chip - 1 - rel], ar_send.at[4 * i + rel], ar_recv.at[4 * i + n_chip - rel], dev(rel, 0))))
        send_bulk(plan[1 + 2 * i])
        total = part_r[k, c] + d2d_r[c]
        for cp in cps[1:] + cps[:1]:
            cp.wait_recv()
        return total + in_r[0] + in_r[2] + in_r[1]

    def gather_rows(i, buf):
        cps = []
        for rel in (OPP, RIGHT, LEFT):
            cps.append(go(rcopy(buf.at[k, c], buf.at[k, c], ag_send.at[8 * i + rel], ag_recv.at[8 * i + n_chip - rel], dev(rel, 0))))
        cps.append(go(rcopy(buf.at[k, c], buf.at[k, c], ag_send.at[8 * i], ag_recv.at[8 * i], dev(0, 1))))
        send_bulk(plan[2 + 2 * i])
        fw = []
        for rel, cp in ((LEFT, cps[1]), (RIGHT, cps[2]), (OPP, cps[0])):
            cp.wait_recv()
            chip = lax.rem(c + rel, n_chip)
            fw.append(go(rcopy(buf.at[k, chip], buf.at[k, chip], ag_send.at[8 * i + 4 + rel], ag_recv.at[8 * i + 4 + rel], dev(0, 1))))
        for cp in [cps[3]] + fw:
            cp.wait_recv()

    ld_wo.wait()
    o_rows = jnp.concatenate([o_all[g * n_row:(g + 1) * n_row] for g in range(heads_loc)], axis=1)
    o_out = dot_f32(o_rows, wo_v[...])
    for p in range(n_dev):
        part[p // n_chip, p % n_chip] = o_out[p * piece:(p + 1) * piece]
    my_piece = pl.ds(pl.multiple_of((k * n_chip + c) * piece, piece), piece)
    att_sum = sum_over_model(0, part, d2d_in, rs_sum, rs_in)
    x1 = (rows_f[my_piece, :] + att_sum).astype(BF16).astype(F32)
    x1_f[...] = x1
    agbuf[k, c] = norm_rows(x1, g_mlp[...].astype(F32)).astype(BF16)
    gather_rows(0, agbuf)
    for p in range(0, n_dev, 2):
        two = [agbuf[i // n_chip, i % n_chip].astype(F32) for i in (p, p + 1)]
        hid_n[pl.ds(p * piece, 2 * piece), :] = jnp.concatenate(two, axis=0).astype(BF16)
    ld_wg.wait()
    ld_wu.wait()
    gate = dot_f32(hid_n[...], wg_v[...])
    up = dot_f32(hid_n[...], wu_v[...])
    mid = (gate * jax.nn.sigmoid(gate) * up).astype(BF16)
    ld_wd.wait()
    down = dot_f32(mid, wd_v[...])
    for p in range(n_dev):
        part2[p // n_chip, p % n_chip] = down[p * piece:(p + 1) * piece]
    mlp_sum = sum_over_model(1, part2, d2d_in2, rs_sum2, rs_in2)
    agbuf2[k, c] = (x1_f[...] + mlp_sum).astype(BF16)
    gather_rows(1, agbuf2)
    send_bulk(len(waiting))
    for p in range(0, n_dev, 2):
        two = jnp.concatenate([agbuf2[i // n_chip, i % n_chip].astype(F32) for i in (p, p + 1)], axis=0).astype(BF16)
        ref, r0 = (last_out, p * piece) if p * piece < n_batch else (dec_out, p * piece - n_batch)
        ref[pl.ds(r0, 2 * piece), :] = two
    for kk in range(2):
        for cp in bulk[kk * 2 * n_bulk:(kk + 1) * 2 * n_bulk]:
            cp.wait_recv()
        put_out(n, slot(OPP, kk), dev(OPP, kk))
        n += 1
    for cp in sends:
        cp.wait_send()
    for cp in outs:
        cp.wait()


def write_kernel(n_part, last_in, dec_in, k_in, v_in, last_out, dec_out, k_out, v_out, tok_v, kv_v, in_sem, out_sem):
    rows = k_in.shape[0] // n_part
    pairs = [(last_in, last_out, tok_v.at[0]), (dec_in, dec_out, tok_v.at[1])]
    for p in range(n_part):
        for i, (src, dst) in enumerate(((k_in, k_out), (v_in, v_out))):
            r = pl.ds(p * rows, rows)
            pairs.append((src.at[r, :], dst.at[r, :], kv_v.at[i, r, :]))
    loads = [pltpu.make_async_copy(src, buf, in_sem.at[n]) for n, (src, dst, buf) in enumerate(pairs)]
    stores = [pltpu.make_async_copy(buf, dst, out_sem.at[n]) for n, (src, dst, buf) in enumerate(pairs)]
    for cp in loads:
        cp.start()
    for ld, st in zip(loads, stores):
        ld.wait()
        st.start()
    for cp in stores:
        cp.wait()


def solution(mesh):
    n_dev = mesh.shape['model']
    assert n_dev == 4 * CORES and mesh.shape['replica'] % 2 == 0
    seq_spec = P('replica', 'model', None)
    col_spec = P(None, None, 'model')
    row_spec = P(None, 'model', None)
    gain_spec = P(None, None)
    tok_spec = P('replica', None)
    cache_spec = P(None, 'replica', None, 'model', None)
    in_specs = (seq_spec, P('replica'), tok_spec, gain_spec, col_spec, col_spec, col_spec, row_spec, gain_spec, col_spec, col_spec, row_spec)
    out_specs = (tok_spec, tok_spec, cache_spec, cache_spec)

    def per_device(prompt, lengths, new_tok, norm_attn, w_q, w_k, w_v, w_o, norm_mlp, w_gate, w_up, w_down):
        assert w_q.shape[0] == 1 and w_k.shape[2] == HEAD_DIM
        n_batch, seq_loc, d_model = prompt.shape
        n_tok = n_batch * seq_loc
        heads_loc = w_q.shape[2] // HEAD_DIM
        ff_loc = w_gate.shape[2]
        n_row = 2 * n_batch
        piece = n_row // n_dev
        n_chip = n_dev // CORES
        hb = n_batch // CORES
        n_q = heads_loc * n_row
        vm = pl.BlockSpec(memory_space=pltpu.VMEM)
        hbm = pl.BlockSpec(memory_space=pl.ANY)
        V = pltpu.VMEM
        DMA = pltpu.SemaphoreType.DMA
        slab = (2, n_tok, HEAD_DIM)
        wide = (CORES, n_chip, piece, d_model)
        n_lr = 2 * pl.cdiv(n_q, HEAD_DIM)
        state = [V((n_q, 1), F32), V((n_q, 1), F32), V((n_q, HEAD_DIM), F32)]
        note = V((2, pl.cdiv(n_q + n_lr, 8) * 8, HEAD_DIM), F32)
        scratch = [
            V((4, seq_loc, d_model), BF16), V((n_tok, d_model), BF16), V((n_dev, d_model, 2 * HEAD_DIM), BF16),
            V((n_dev - 1,) + slab, BF16), V((n_dev,) + slab, BF16),
            V((d_model, heads_loc * HEAD_DIM), BF16), V((d_model, ff_loc), BF16), V((d_model, ff_loc), BF16),
            V((n_tok, HEAD_DIM), F32), V((n_tok, HEAD_DIM), F32),
            V((n_batch, HEAD_DIM), jnp.int32), V((seq_loc, HEAD_DIM), F32), V((seq_loc, HEAD_DIM), F32), V((n_row, HEAD_DIM), F32), V((n_row, HEAD_DIM), F32),
            V((n_batch, d_model), F32), V((n_batch, d_model), BF16), V((n_batch, d_model), BF16), V((hb, d_model), BF16),
            V((n_chip - 1, hb, d_model), BF16), V((hb, d_model), BF16), V((hb, d_model), BF16),
            V((n_row, d_model), F32), V((n_row, d_model), BF16), V((n_q, HEAD_DIM), BF16), V((2, n_q, HEAD_DIM), BF16),
            V((n_batch, HEAD_DIM), BF16), V((n_batch, HEAD_DIM), BF16),
            *state, *state, note, note,
            V(wide, F32), V(wide[1:], F32), V(wide[1:], F32), V((n_chip - 1,) + wide[2:], F32), V(wide, BF16), V(wide[2:], F32),
            V((n_row, d_model), BF16),
            V(wide, F32), V(wide[1:], F32), V(wide[1:], F32), V((n_chip - 1,) + wide[2:], F32), V(wide, BF16),
            DMA((4,)), DMA((5,)), DMA((25,)), DMA((4 * n_dev,)), DMA((5,)), DMA((n_dev,)), DMA((4 * N_BULK,)), DMA((4 * N_BULK,)), DMA((4,)), DMA((4,)),
            DMA((5,)), DMA((5,)), DMA((2 + 2 * n_dev,)), DMA((8,)), DMA((8,)), DMA((16,)), DMA((16,)),
        ]
        cache_rows = (seq_loc * n_dev + 1) * n_batch
        cache = jax.ShapeDtypeStruct((cache_rows, HEAD_DIM), BF16)
        tok = jax.ShapeDtypeStruct((n_batch, d_model), BF16)
        made = pl.pallas_call(
            functools.partial(kernel, n_dev, n_batch, seq_loc, d_model, heads_loc, ff_loc, N_BULK, PLAN),
            out_shape=[tok, tok, cache, cache],
            in_specs=[pl.BlockSpec(memory_space=pltpu.SMEM), hbm] + [vm] * 3 + [hbm] * 7,
            out_specs=[vm, vm, hbm, hbm],
            scratch_shapes=scratch,
            compiler_params=pltpu.CompilerParams(collective_id=0, has_side_effects=True, vmem_limit_bytes=67_043_328),
        )(lengths, prompt, new_tok, norm_attn, norm_mlp, w_q[0], w_k[0], w_v[0], w_o[0], w_gate[0], w_up[0], w_down[0])
        n_part = next(p for p in range(4, cache_rows) if cache_rows // n_batch % p == 0)
        last, dec, kc, vc = pl.pallas_call(
            functools.partial(write_kernel, n_part),
            out_shape=[tok, tok, cache, cache],
            in_specs=[hbm] * 4,
            out_specs=[hbm] * 4,
            scratch_shapes=[V((2, n_batch, d_model), BF16), V((2, cache_rows, HEAD_DIM), BF16), DMA((2 + 2 * n_part,)), DMA((2 + 2 * n_part,))],
        )(*made)

        def as_cache(arr):
            return jnp.transpose(arr.reshape(1, seq_loc * n_dev + 1, 1, n_batch, HEAD_DIM), (0, 3, 1, 2, 4))

        return dec, last, as_cache(kc), as_cache(vc)

    return jax.shard_map(per_device, mesh=mesh, in_specs=in_specs, out_specs=out_specs, check_vma=False)
```

```python
import functools
import math

import jax
import jax.numpy as jnp
from jax import lax
from jax.experimental import pallas as pl
from jax.experimental.pallas import tpu as pltpu
from jax.sharding import PartitionSpec as P

HEAD_DIM = 128
NEG_BIG = -1e30
CORES = 2
N_BULK = 2
PLAN = (2, 1, 3, 1, 1)
MESH_ID = pl.DeviceIdType.MESH
BF16 = jnp.bfloat16
F32 = jnp.float32


def dot_f32(a, b):
    return jnp.dot(a, b, preferred_element_type=F32)


def dot_bt(a, b):
    return lax.dot_general(a, b, (((1,), (1,)), ((), ())), preferred_element_type=F32)


def norm_rows(x_f32, gain_f32):
    inv_rms = lax.rsqrt(jnp.mean(x_f32 * x_f32, axis=-1, keepdims=True) + 1e-5)
    return x_f32 * inv_rms * gain_f32


def rotate(x_f32, cos_full, sin_signed):
    return x_f32 * cos_full + pltpu.roll(x_f32, HEAD_DIM // 2, 1) * sin_signed


def kernel(n_dev, n_batch, seq_loc, d_model, heads_loc, ff_loc, n_bulk, plan,
           lens, prompt, new_tok, g_attn, g_mlp, wq, wk, wv, wo, wg, wu, wd,
           last_out, dec_out, kvrecv, kvnew,
           xbuf, normed, wbuf, stage, wq_v, wg_v, wu_v, res_k, res_v,
           len_v, cos_pos, sin_pos, cos_row, sin_row,
           last_f, xl_own, xl_sib, xl_sum, xl_recv, xl_half, xl_oth, rows_f, rows_n, q_s, q_in,
           m_s, l_s, acc_s, m_p, l_p, acc_p, msg, msg_in,
           part, d2d_in, rs_sum, rs_in, agbuf, x1_f, hid_n, part2, d2d_in2, rs_sum2, rs_in2, agbuf2,
           xsem, ldsem, w_send, w_recv, kv_send, kv_recv, bulk_send, bulk_recv, pt_send, pt_recv, xl_send, xl_rsem,
           ar_send, ar_recv, ag_send, ag_recv):
    n_chip = n_dev // CORES
    n_tok = n_batch * seq_loc
    n_row = 2 * n_batch
    piece = n_row // n_dev
    quarter = d_model // 4
    me = lax.axis_index('model')
    c = me // CORES
    k = me % CORES
    o_core = 1 - k
    replica = lax.axis_index('replica')
    odd = lax.rem(replica, 2)
    partner = {'replica': replica + 1 - 2 * odd}

    def dev(rel, kk):
        chip = lax.rem(c + rel, n_chip)
        return CORES * chip + (k if kk == 0 else o_core)

    RIGHT, OPP, LEFT = 1, 2, 3

    def slot(rel, kk):
        return rel * CORES + kk

    def rcopy(src, dst, ssem, rsem, target):
        target = target if isinstance(target, dict) else {'model': target}
        return pltpu.make_async_remote_copy(src_ref=src, dst_ref=dst, send_sem=ssem, recv_sem=rsem,
                                            device_id=target, device_id_type=MESH_ID)

    own_w = slot(0, 0)
    ld_wk = pltpu.make_async_copy(wk, wbuf.at[own_w, :, pl.ds(0, HEAD_DIM)], ldsem.at[0])
    ld_wv = pltpu.make_async_copy(wv, wbuf.at[own_w, :, pl.ds(HEAD_DIM, HEAD_DIM)], ldsem.at[1])
    ld_wk.start()
    ld_wv.start()
    n_x = xbuf.shape[0]

    def x_copy(b, s):
        return pltpu.make_async_copy(prompt.at[b], xbuf.at[s], xsem.at[s])

    for b in range(n_x - 1):
        x_copy(b, b).start()

    barrier = pltpu.get_barrier_semaphore()
    for d in range(1, n_dev):
        pl.semaphore_signal(barrier, inc=1, device_id={'model': lax.rem(me + d, n_dev)}, device_id_type=MESH_ID)
    pl.semaphore_signal(barrier, inc=1, device_id=partner, device_id_type=MESH_ID)
    pl.semaphore_wait(barrier, n_dev)

    order = [i + odd * (3 - 2 * i) for i in range(4)]

    def w_part(sl, i):
        return wbuf.at[sl, pl.ds(pl.multiple_of(order[i] * quarter, quarter), quarter), :]

    def w_copy(n, src_slot, dst_slot, i, target, i_there=None):
        sem = w_recv.at[dst_slot * 4 + (i if i_there is None else i_there)]
        return rcopy(w_part(src_slot, i), w_part(dst_slot, i), w_send.at[n], sem, target)

    ld_wk.wait()
    ld_wv.wait()
    sends = []

    def go(cp):
        cp.start()
        sends.append(cp)
        return cp

    to_r = [w_copy(i, own_w, slot(LEFT, 0), i, dev(RIGHT, 0)) for i in range(3)]
    to_l = [w_copy(3 + i, own_w, slot(RIGHT, 0), i, dev(LEFT, 0)) for i in range(3)]
    to_s = rcopy(wbuf.at[own_w], wbuf.at[slot(0, 1)], w_send.at[6], w_recv.at[slot(0, 1) * 4], dev(0, 1))
    for cp in (to_r[0], to_l[0], to_r[1], to_l[1], to_s):
        go(cp)
    fwd_r = w_copy(7, slot(LEFT, 0), slot(OPP, 0), 0, dev(RIGHT, 0))
    fwd_l = w_copy(8, slot(RIGHT, 0), slot(OPP, 0), 1, dev(LEFT, 0))
    to_p = {(rel, i): w_copy(9 + n, slot(rel, 0), slot(rel, 0), i, partner, 3 - i)
            for n, (rel, i) in enumerate(((LEFT, 0), (RIGHT, 0), (OPP, 0), (OPP, 1)))}
    sib_fwd = {(rel, i): w_copy(13 + 4 * n + i, slot(rel, 0), slot(rel, 1), i, dev(0, 1))
               for n, rel in enumerate((LEFT, RIGHT, OPP)) for i in range(4)}

    ld_wq = pltpu.make_async_copy(wq, wq_v, ldsem.at[2])
    ld_wg = pltpu.make_async_copy(wg, wg_v, ldsem.at[3])
    ld_wu = pltpu.make_async_copy(wu, wu_v, ldsem.at[4])

    gain = g_attn[...].astype(F32)
    pos0 = me * seq_loc

    @pl.loop(0, n_batch)
    def _(b):
        s = lax.rem(b, n_x)

        @pl.when(b + n_x - 1 < n_batch)
        def _():
            x_copy(b + n_x - 1, lax.rem(b + n_x - 1, n_x)).start()

        x_copy(b, s).wait()
        x = xbuf[s].astype(F32)
        normed[pl.ds(pl.multiple_of(b * seq_loc, seq_loc), seq_loc), :] = norm_rows(x, gain).astype(BF16)
        here = (lax.broadcasted_iota(jnp.int32, (seq_loc, 1), 0) + pos0 == lens[b] - 1).astype(F32)
        last_f[pl.ds(b, 1), :] = jnp.sum(x * here, axis=0, keepdims=True)
        len_v[pl.ds(b, 1), :] = jnp.full((1, HEAD_DIM), lens[b], jnp.int32)

    ld_wq.start()
    ld_wg.start()
    ld_wu.start()

    xl_own[...] = last_f[...].astype(BF16)
    xl_a = go(rcopy(xl_own, xl_sib, xl_send.at[0], xl_rsem.at[0], dev(0, 1)))

    def table(cos_ref, sin_ref, rows, pos):
        lane = lax.broadcasted_iota(jnp.int32, pos.shape, 1)
        hd = HEAD_DIM // 2
        step = jnp.where(lane < hd, lane, lane - hd).astype(F32)
        angle = pos.astype(F32) * jnp.exp(step * (-2.0 * math.log(10000.0) / HEAD_DIM))
        cos_ref[rows, :] = jnp.cos(angle)
        sin_ref[rows, :] = jnp.where(lane < hd, -1.0, 1.0) * jnp.sin(angle)

    table(cos_pos, sin_pos, pl.ds(0, seq_loc), lax.broadcasted_iota(jnp.int32, (seq_loc, HEAD_DIM), 0) + pos0)
    table(cos_row, sin_row, pl.ds(0, n_batch), len_v[...] - 1)
    table(cos_row, sin_row, pl.ds(n_batch, n_batch), len_v[...])

    hb = n_batch // CORES
    xl_a.wait_recv()
    my_rows = pl.ds(pl.multiple_of(k * hb, hb), hb)
    oth_rows = pl.ds(pl.multiple_of(o_core * hb, hb), hb)
    xl_sum[...] = xl_own[my_rows, :] + xl_sib[my_rows, :]
    xl_b = [go(rcopy(xl_sum, xl_recv.at[n_chip - 1 - rel], xl_send.at[rel], xl_rsem.at[n_chip - rel], dev(rel, 0))) for rel in (RIGHT, LEFT, OPP)]
    go(to_r[2])
    go(to_l[2])

    def head(sl, dst):
        for_rows = 512

        @pl.loop(0, n_tok // for_rows)
        def _(m):
            r0 = pl.multiple_of(m * for_rows, for_rows)
            res = dot_f32(normed[pl.ds(r0, for_rows), :], wbuf[sl])
            res_k[pl.ds(r0, for_rows), :] = res[:, :HEAD_DIM]
            res_v[pl.ds(r0, for_rows), :] = res[:, HEAD_DIM:]

        @pl.loop(0, seq_loc, unroll=4)
        def _(s):
            rows = pl.ds(pl.multiple_of(s * n_batch, n_batch), n_batch)
            kt = res_k[pl.ds(s, n_batch, stride=seq_loc), :]
            dst[0, rows, :] = rotate(kt, cos_pos[pl.ds(s, 1), :], sin_pos[pl.ds(s, 1), :]).astype(BF16)
            dst[1, rows, :] = res_v[pl.ds(s, n_batch, stride=seq_loc), :].astype(BF16)

    def kv_copy(n, rel, kk):
        sl = slot((n_chip - rel) % n_chip, kk)
        return rcopy(stage.at[slot(rel, kk) - 1], kvrecv.at[sl], kv_send.at[n], kv_recv.at[sl], dev(rel, kk))

    def wait_w(rel, kk, i):
        w_copy(0, slot(rel, kk), slot(rel, kk), i, dev(0, 1)).wait_recv()

    for rel in (LEFT, RIGHT):
        wait_w(rel, 0, 0)
        go(to_p[rel, 0])
        go(sib_fwd[rel, 0])
        if rel == LEFT:
            go(fwd_r)
    head(own_w, kvrecv.at[own_w])
    for rel in (RIGHT, LEFT):
        wait_w(rel, 0, 1)
        if rel == RIGHT:
            go(fwd_l)
        go(sib_fwd[rel, 1])
    to_s.wait_recv()
    head(slot(0, 1), stage.at[slot(0, 1) - 1])
    kv_sib = go(kv_copy(0, 0, 1))

    for cp in xl_b:
        cp.wait_recv()
    xl_half[...] = xl_sum[...] + xl_recv[0] + (xl_recv[1] + xl_recv[2])
    xl_c = go(rcopy(xl_half, xl_oth, xl_send.at[4], xl_rsem.at[4], dev(0, 1)))

    rows_f[my_rows, :] = xl_half[...].astype(F32)
    rows_f[pl.ds(n_batch, n_batch), :] = new_tok[...].astype(F32)
    ld_wq.wait()
    xl_c.wait_recv()
    rows_f[oth_rows, :] = xl_oth[...].astype(F32)
    rows_n[...] = norm_rows(rows_f[...], gain).astype(BF16)
    q_all = dot_f32(rows_n[...], wq_v[...])
    for g in range(heads_loc):
        q_g = rotate(q_all[:, g * HEAD_DIM:(g + 1) * HEAD_DIM], cos_row[...], sin_row[...])
        q_s[pl.ds(g * n_row, n_row), :] = q_g.astype(BF16)
    q_out = [go(rcopy(q_s, q_in.at[kk], pt_send.at[kk], pt_recv.at[kk], dev(OPP, kk))) for kk in range(2)]
    kv_new = dot_f32(rows_n[...], wbuf[own_w])
    new_rows = slice(n_batch, n_row)
    k_new = rotate(kv_new[new_rows, :HEAD_DIM], cos_row[pl.ds(n_batch, n_batch), :], sin_row[pl.ds(n_batch, n_batch), :])
    kvnew[0] = k_new.astype(BF16)
    kvnew[1] = kv_new[new_rows, HEAD_DIM:].astype(BF16)

    for rel in (LEFT, RIGHT):
        for i in (3, 2):
            wait_w(rel, 0, i)
            go(sib_fwd[rel, i])
    n = 1
    kv_nb = {}
    for kk in range(2):
        for rel in (RIGHT, LEFT):
            if kk == 1:
                for i in range(4):
                    wait_w(rel, 1, i)
            head(slot(rel, kk), stage.at[slot(rel, kk) - 1])
            kv_nb[rel, kk] = go(kv_copy(n, rel, kk))
            n += 1
        if kk == 0:
            for i in range(2):
                wait_w(OPP, 0, i)
                go(to_p[OPP, i])
                go(sib_fwd[OPP, i])

    scale = HEAD_DIM ** -0.5
    n_q = heads_loc * n_row
    chunk = min(512, n_tok)
    mine = (m_s, l_s, acc_s)

    def reset(state):
        state[0][...] = jnp.full(state[0].shape, NEG_BIG, F32)
        state[1][...] = jnp.zeros(state[1].shape, F32)
        state[2][...] = jnp.zeros(state[2].shape, F32)

    def update(state, sc, valid, v_blk):
        m_r, l_r, acc_r = state
        sc = jnp.where(valid, sc * scale, NEG_BIG)
        m_old = m_r[...]
        m_new = jnp.maximum(m_old, jnp.max(sc, axis=-1, keepdims=True))
        prob = jnp.where(valid, jnp.exp(sc - m_new), 0.0)
        alpha = jnp.exp(m_old - m_new)
        l_r[...] = l_r[...] * alpha + jnp.sum(prob, axis=-1, keepdims=True)
        acc_r[...] = acc_r[...] * alpha + dot_f32(prob.astype(BF16), v_blk)
        m_r[...] = m_new

    def attend(state, q_ref, kv_ref, src):
        @pl.loop(0, n_tok // chunk)
        def _(ch):
            rows = pl.ds(pl.multiple_of(ch * chunk, chunk), chunk)
            sc = dot_bt(q_ref[...], kv_ref[0, rows, :])
            col = lax.broadcasted_iota(jnp.int32, (n_q, chunk), 1)
            row = lax.broadcasted_iota(jnp.int32, (n_q, chunk), 0)
            pos = src * seq_loc + ch * (chunk // n_batch) + col // n_batch
            len_row = jnp.concatenate([len_v[:, :1]] * (n_q // n_batch), axis=0)
            valid = (col % n_batch == row % n_batch) & (pos < len_row)
            update(state, sc, valid, kv_ref[1, rows, :])

    lane_rows = [(i, min(HEAD_DIM, n_q - i)) for i in range(0, n_q, HEAD_DIM)]

    def on_diag(size):
        return lax.broadcasted_iota(jnp.int32, (size, HEAD_DIM), 0) == lax.broadcasted_iota(jnp.int32, (size, HEAD_DIM), 1)

    def put_column(ref, r0, column):
        for j, (i, size) in enumerate(lane_rows):
            ref[pl.ds(r0 + j, 1), :] = jnp.sum(jnp.where(on_diag(size), column[i:i + size], 0.0), axis=0, keepdims=True)

    def get_column(ref, r0):
        cols = [jnp.sum(jnp.where(on_diag(size), ref[pl.ds(r0 + j, 1), :], 0.0), axis=1, keepdims=True) for j, (i, size) in enumerate(lane_rows)]
        return jnp.concatenate(cols, axis=0)

    reset(mine)
    col = lax.broadcasted_iota(jnp.int32, (n_q, n_batch), 1)
    row = lax.broadcasted_iota(jnp.int32, (n_q, n_batch), 0)
    is_new = (row // n_batch) % 2 == 1
    update(mine, dot_bt(q_s[...], kvnew[0]), (col == row % n_batch) & is_new, kvnew[1])
    attend(mine, q_s, kvrecv.at[own_w], me)
    kv_sib.wait_recv()
    attend(mine, q_s, kvrecv.at[slot(0, 1)], dev(0, 1))

    n_lr = len(lane_rows)
    pt_out = []
    for i in (3, 2):
        wait_w(OPP, 0, i)
        go(sib_fwd[OPP, i])
    for kk in range(2):
        if kk == 1:
            for i in range(4):
                wait_w(OPP, 1, i)
        block = stage.at[slot(OPP, kk) - 1]
        head(slot(OPP, kk), block)
        q_out[kk].wait_recv()
        other = (m_p, l_p, acc_p)
        reset(other)
        attend(other, q_in.at[kk], block, me)
        msg[kk, pl.ds(0, n_q), :] = acc_p[...]
        put_column(msg.at[kk], n_q, m_p[...])
        put_column(msg.at[kk], n_q + n_lr, l_p[...])
        pt_out.append(go(rcopy(msg.at[kk], msg_in.at[kk], pt_send.at[2 + kk], pt_recv.at[2 + kk], dev(OPP, kk))))

    per = n_tok // n_bulk
    bulk = []
    for kk in range(2):
        for i in range(2):
            for j in range(n_bulk):
                rows = pl.ds(j * per, per)
                x = len(bulk)
                bulk.append(rcopy(stage.at[slot(OPP, kk) - 1, i, rows, :], kvrecv.at[slot(OPP, kk), i, rows, :], bulk_send.at[x], bulk_recv.at[x], dev(OPP, kk)))
    waiting = list(bulk)

    def send_bulk(count):
        for _ in range(count):
            if waiting:
                go(waiting.pop(0))

    send_bulk(plan[0])

    wd_v = normed.at[pl.ds(0, ff_loc), :]
    wo_v = normed.at[pl.ds(ff_loc, heads_loc * HEAD_DIM), :]
    ld_wo = pltpu.make_async_copy(wo, wo_v, ldsem.at[0])
    ld_wd = pltpu.make_async_copy(wd, wd_v, ldsem.at[1])
    ld_wo.start()
    ld_wd.start()

    n = 2
    for kk in range(2):
        for rel in (RIGHT, LEFT):
            src_rel = (n_chip - rel) % n_chip
            kv_nb[rel, kk].wait_recv()
            attend(mine, q_s, kvrecv.at[slot(src_rel, kk)], dev(src_rel, kk))
            n += 1
    for kk in range(2):
        pt_out[kk].wait_recv()
        m_o = get_column(msg_in.at[kk], n_q)
        l_o = get_column(msg_in.at[kk], n_q + n_lr)
        m_old = m_s[...]
        m_new = jnp.maximum(m_old, m_o)
        f_mine, f_oth = jnp.exp(m_old - m_new), jnp.exp(m_o - m_new)
        l_s[...] = l_s[...] * f_mine + l_o * f_oth
        acc_s[...] = acc_s[...] * f_mine + msg_in[kk, pl.ds(0, n_q), :] * f_oth
        m_s[...] = m_new
    o_all = (acc_s[...] / l_s[...]).astype(BF16)

    def sum_over_model(i, part_r, d2d_r, sum_r, in_r):
        cp = go(rcopy(part_r.at[o_core], d2d_r, ar_send.at[4 * i], ar_recv.at[4 * i], dev(0, 1)))
        cp.wait_recv()
        cps = []
        for rel in (OPP, RIGHT, LEFT):
            chip = lax.rem(c + rel, n_chip)
            sum_r[rel] = part_r[k, chip] + d2d_r[chip]
            cps.append(go(rcopy(sum_r.at[rel], in_r.at[n_chip - 1 - rel], ar_send.at[4 * i + rel], ar_recv.at[4 * i + n_chip - rel], dev(rel, 0))))
        send_bulk(plan[1 + 2 * i])
        total = part_r[k, c] + d2d_r[c]
        for cp in cps[1:] + cps[:1]:
            cp.wait_recv()
        return total + in_r[0] + in_r[2] + in_r[1]

    def gather_rows(i, buf):
        cps = []
        for rel in (OPP, RIGHT, LEFT):
            cps.append(go(rcopy(buf.at[k, c], buf.at[k, c], ag_send.at[8 * i + rel], ag_recv.at[8 * i + n_chip - rel], dev(rel, 0))))
        cps.append(go(rcopy(buf.at[k, c], buf.at[k, c], ag_send.at[8 * i], ag_recv.at[8 * i], dev(0, 1))))
        send_bulk(plan[2 + 2 * i])
        fw = []
        for rel, cp in ((LEFT, cps[1]), (RIGHT, cps[2]), (OPP, cps[0])):
            cp.wait_recv()
            chip = lax.rem(c + rel, n_chip)
            fw.append(go(rcopy(buf.at[k, chip], buf.at[k, chip], ag_send.at[8 * i + 4 + rel], ag_recv.at[8 * i + 4 + rel], dev(0, 1))))
        for cp in [cps[3]] + fw:
            cp.wait_recv()

    ld_wo.wait()
    o_rows = jnp.concatenate([o_all[g * n_row:(g + 1) * n_row] for g in range(heads_loc)], axis=1)
    o_out = dot_f32(o_rows, wo_v[...])
    for p in range(n_dev):
        part[p // n_chip, p % n_chip] = o_out[p * piece:(p + 1) * piece]
    my_piece = pl.ds(pl.multiple_of((k * n_chip + c) * piece, piece), piece)
    att_sum = sum_over_model(0, part, d2d_in, rs_sum, rs_in)
    x1 = (rows_f[my_piece, :] + att_sum).astype(BF16).astype(F32)
    x1_f[...] = x1
    agbuf[k, c] = norm_rows(x1, g_mlp[...].astype(F32)).astype(BF16)
    gather_rows(0, agbuf)
    for p in range(0, n_dev, 2):
        two = [agbuf[i // n_chip, i % n_chip].astype(F32) for i in (p, p + 1)]
        hid_n[pl.ds(p * piece, 2 * piece), :] = jnp.concatenate(two, axis=0).astype(BF16)
    ld_wg.wait()
    ld_wu.wait()
    gate = dot_f32(hid_n[...], wg_v[...])
    up = dot_f32(hid_n[...], wu_v[...])
    mid = (gate * jax.nn.sigmoid(gate) * up).astype(BF16)
    ld_wd.wait()
    down = dot_f32(mid, wd_v[...])
    for p in range(n_dev):
        part2[p // n_chip, p % n_chip] = down[p * piece:(p + 1) * piece]
    mlp_sum = sum_over_model(1, part2, d2d_in2, rs_sum2, rs_in2)
    agbuf2[k, c] = (x1_f[...] + mlp_sum).astype(BF16)
    gather_rows(1, agbuf2)
    send_bulk(len(waiting))
    for p in range(0, n_dev, 2):
        two = jnp.concatenate([agbuf2[i // n_chip, i % n_chip].astype(F32) for i in (p, p + 1)], axis=0).astype(BF16)
        ref, r0 = (last_out, p * piece) if p * piece < n_batch else (dec_out, p * piece - n_batch)
        ref[pl.ds(r0, 2 * piece), :] = two
    for kk in range(2):
        for cp in bulk[kk * 2 * n_bulk:(kk + 1) * 2 * n_bulk]:
            cp.wait_recv()
        n += 1
    for cp in sends:
        cp.wait_send()


def write_kernel(n_dev, last_in, dec_in, kv, kv_new, last_out, dec_out, k_out, v_out, sem):
    n_tok = kv.shape[2]
    n_batch = kv_new.shape[1]
    me = lax.axis_index('model')
    pairs = [(last_in, last_out), (dec_in, dec_out)]
    for i, ref in enumerate((k_out, v_out)):
        pairs.append((kv_new.at[i], ref.at[pl.ds(n_dev * n_tok, n_batch), :]))
        for sl in range(n_dev):
            chip = lax.rem(me // CORES + sl // CORES, n_dev // CORES)
            core = lax.rem(me + sl, CORES)
            src = pl.ds(pl.multiple_of((CORES * chip + core) * n_tok, n_tok), n_tok)
            pairs.append((kv.at[sl, i], ref.at[src, :]))
    copies = [pltpu.make_async_copy(src, dst, sem.at[n]) for n, (src, dst) in enumerate(pairs)]
    for cp in copies:
        cp.start()
    for cp in copies:
        cp.wait()


def solution(mesh):
    n_dev = mesh.shape['model']
    assert n_dev == 4 * CORES and mesh.shape['replica'] % 2 == 0
    seq_spec = P('replica', 'model', None)
    col_spec = P(None, None, 'model')
    row_spec = P(None, 'model', None)
    gain_spec = P(None, None)
    tok_spec = P('replica', None)
    cache_spec = P(None, 'replica', None, 'model', None)
    in_specs = (seq_spec, P('replica'), tok_spec, gain_spec, col_spec, col_spec, col_spec, row_spec, gain_spec, col_spec, col_spec, row_spec)
    out_specs = (tok_spec, tok_spec, cache_spec, cache_spec)

    def per_device(prompt, lengths, new_tok, norm_attn, w_q, w_k, w_v, w_o, norm_mlp, w_gate, w_up, w_down):
        assert w_q.shape[0] == 1 and w_k.shape[2] == HEAD_DIM
        n_batch, seq_loc, d_model = prompt.shape
        n_tok = n_batch * seq_loc
        heads_loc = w_q.shape[2] // HEAD_DIM
        ff_loc = w_gate.shape[2]
        n_row = 2 * n_batch
        piece = n_row // n_dev
        n_chip = n_dev // CORES
        hb = n_batch // CORES
        n_q = heads_loc * n_row
        vm = pl.BlockSpec(memory_space=pltpu.VMEM)
        hbm = pl.BlockSpec(memory_space=pl.ANY)
        V = pltpu.VMEM
        DMA = pltpu.SemaphoreType.DMA
        slab = (2, n_tok, HEAD_DIM)
        wide = (CORES, n_chip, piece, d_model)
        n_lr = 2 * pl.cdiv(n_q, HEAD_DIM)
        state = [V((n_q, 1), F32), V((n_q, 1), F32), V((n_q, HEAD_DIM), F32)]
        note = V((2, pl.cdiv(n_q + n_lr, 8) * 8, HEAD_DIM), F32)
        scratch = [
            V((4, seq_loc, d_model), BF16), V((n_tok, d_model), BF16), V((n_dev, d_model, 2 * HEAD_DIM), BF16),
            V((n_dev - 1,) + slab, BF16),
            V((d_model, heads_loc * HEAD_DIM), BF16), V((d_model, ff_loc), BF16), V((d_model, ff_loc), BF16),
            V((n_tok, HEAD_DIM), F32), V((n_tok, HEAD_DIM), F32),
            V((n_batch, HEAD_DIM), jnp.int32), V((seq_loc, HEAD_DIM), F32), V((seq_loc, HEAD_DIM), F32), V((n_row, HEAD_DIM), F32), V((n_row, HEAD_DIM), F32),
            V((n_batch, d_model), F32), V((n_batch, d_model), BF16), V((n_batch, d_model), BF16), V((hb, d_model), BF16),
            V((n_chip - 1, hb, d_model), BF16), V((hb, d_model), BF16), V((hb, d_model), BF16),
            V((n_row, d_model), F32), V((n_row, d_model), BF16), V((n_q, HEAD_DIM), BF16), V((2, n_q, HEAD_DIM), BF16),
            *state, *state, note, note,
            V(wide, F32), V(wide[1:], F32), V(wide[1:], F32), V((n_chip - 1,) + wide[2:], F32), V(wide, BF16), V(wide[2:], F32),
            V((n_row, d_model), BF16),
            V(wide, F32), V(wide[1:], F32), V(wide[1:], F32), V((n_chip - 1,) + wide[2:], F32), V(wide, BF16),
            DMA((4,)), DMA((5,)), DMA((25,)), DMA((4 * n_dev,)), DMA((5,)), DMA((n_dev,)), DMA((4 * N_BULK,)), DMA((4 * N_BULK,)), DMA((4,)), DMA((4,)),
            DMA((5,)), DMA((5,)), DMA((8,)), DMA((8,)), DMA((16,)), DMA((16,)),
        ]
        cache_rows = (seq_loc * n_dev + 1) * n_batch
        cache = jax.ShapeDtypeStruct((cache_rows, HEAD_DIM), BF16)
        tok = jax.ShapeDtypeStruct((n_batch, d_model), BF16)
        made = pl.pallas_call(
            functools.partial(kernel, n_dev, n_batch, seq_loc, d_model, heads_loc, ff_loc, N_BULK, PLAN),
            out_shape=[V((n_batch, d_model), BF16), V((n_batch, d_model), BF16), V((n_dev,) + slab, BF16), V((2, n_batch, HEAD_DIM), BF16)],
            in_specs=[pl.BlockSpec(memory_space=pltpu.SMEM), hbm] + [vm] * 3 + [hbm] * 7,
            out_specs=[vm] * 4,
            scratch_shapes=scratch,
            compiler_params=pltpu.CompilerParams(collective_id=0, has_side_effects=True, vmem_limit_bytes=60_300_000),
        )(lengths, prompt, new_tok, norm_attn, norm_mlp, w_q[0], w_k[0], w_v[0], w_o[0], w_gate[0], w_up[0], w_down[0])
        last, dec, kc, vc = pl.pallas_call(
            functools.partial(write_kernel, n_dev),
            out_shape=[tok, tok, cache, cache],
            in_specs=[vm] * 4,
            out_specs=[hbm] * 4,
            scratch_shapes=[DMA((4 + 2 * n_dev,))],
            compiler_params=pltpu.CompilerParams(vmem_limit_bytes=1 << 20),
        )(*made)

        def as_cache(arr):
            return jnp.transpose(arr.reshape(1, seq_loc * n_dev + 1, 1, n_batch, HEAD_DIM), (0, 3, 1, 2, 4))

        return dec, last, as_cache(kc), as_cache(vc)

    return jax.shard_map(per_device, mesh=mesh, in_specs=in_specs, out_specs=out_specs, check_vma=False)
```

```python
import functools
import math

import jax
import jax.numpy as jnp
from jax import lax
from jax.experimental import pallas as pl
from jax.experimental.pallas import tpu as pltpu
from jax.sharding import PartitionSpec as P

HEAD_DIM = 128
NEG_BIG = -1e30
CORES = 2
N_BULK = 2
PLAN = (2, 1, 3, 1, 1)
MESH_ID = pl.DeviceIdType.MESH
BF16 = jnp.bfloat16
F32 = jnp.float32


def dot_f32(a, b):
    return jnp.dot(a, b, preferred_element_type=F32)


def dot_bt(a, b):
    return lax.dot_general(a, b, (((1,), (1,)), ((), ())), preferred_element_type=F32)


def norm_rows(x_f32, gain_f32):
    inv_rms = lax.rsqrt(jnp.mean(x_f32 * x_f32, axis=-1, keepdims=True) + 1e-5)
    return x_f32 * inv_rms * gain_f32


def rotate(x_f32, cos_full, sin_signed):
    return x_f32 * cos_full + pltpu.roll(x_f32, HEAD_DIM // 2, 1) * sin_signed


def kernel(n_dev, n_batch, seq_loc, d_model, heads_loc, ff_loc, n_bulk, plan,
           lens, prompt, new_tok, g_attn, g_mlp, wq, wk, wv, wo, wg, wu, wd,
           last_out, dec_out, kvrecv, kvnew,
           xbuf, normed, wbuf, stage, wq_v, wg_v, wu_v, res_k, res_v,
           len_v, cos_pos, sin_pos, cos_row, sin_row,
           last_f, xl_own, xl_sib, xl_sum, xl_recv, xl_half, xl_oth, rows_f, rows_n, q_s, q_in,
           m_s, l_s, acc_s, m_p, l_p, acc_p, msg, msg_in,
           part, d2d_in, rs_sum, rs_in, agbuf, x1_f, hid_n, part2, d2d_in2, rs_sum2, rs_in2, agbuf2,
           xsem, ldsem, w_send, w_recv, kv_send, kv_recv, bulk_send, bulk_recv, pt_send, pt_recv, xl_send, xl_rsem,
           ar_send, ar_recv, ag_send, ag_recv):
    n_chip = n_dev // CORES
    n_tok = n_batch * seq_loc
    n_row = 2 * n_batch
    piece = n_row // n_dev
    quarter = d_model // 4
    me = lax.axis_index('model')
    c = me // CORES
    k = me % CORES
    o_core = 1 - k
    replica = lax.axis_index('replica')
    odd = lax.rem(replica, 2)
    partner = {'replica': replica + 1 - 2 * odd}

    def dev(rel, kk):
        chip = lax.rem(c + rel, n_chip)
        return CORES * chip + (k if kk == 0 else o_core)

    RIGHT, OPP, LEFT = 1, 2, 3

    def slot(rel, kk):
        return rel * CORES + kk

    def rcopy(src, dst, ssem, rsem, target):
        target = target if isinstance(target, dict) else {'model': target}
        return pltpu.make_async_remote_copy(src_ref=src, dst_ref=dst, send_sem=ssem, recv_sem=rsem,
                                            device_id=target, device_id_type=MESH_ID)

    own_w = slot(0, 0)
    ld_wk = pltpu.make_async_copy(wk, wbuf.at[own_w, :, pl.ds(0, HEAD_DIM)], ldsem.at[0])
    ld_wv = pltpu.make_async_copy(wv, wbuf.at[own_w, :, pl.ds(HEAD_DIM, HEAD_DIM)], ldsem.at[1])
    ld_wk.start()
    ld_wv.start()
    n_x = xbuf.shape[0]

    def x_copy(b, s):
        return pltpu.make_async_copy(prompt.at[b], xbuf.at[s], xsem.at[s])

    for b in range(n_x - 1):
        x_copy(b, b).start()

    barrier = pltpu.get_barrier_semaphore()
    for d in range(1, n_dev):
        pl.semaphore_signal(barrier, inc=1, device_id={'model': lax.rem(me + d, n_dev)}, device_id_type=MESH_ID)
    pl.semaphore_signal(barrier, inc=1, device_id=partner, device_id_type=MESH_ID)
    pl.semaphore_wait(barrier, n_dev)

    order = [i + odd * (3 - 2 * i) for i in range(4)]

    def w_part(sl, i):
        return wbuf.at[sl, pl.ds(pl.multiple_of(order[i] * quarter, quarter), quarter), :]

    def w_copy(n, src_slot, dst_slot, i, target, i_there=None):
        sem = w_recv.at[dst_slot * 4 + (i if i_there is None else i_there)]
        return rcopy(w_part(src_slot, i), w_part(dst_slot, i), w_send.at[n], sem, target)

    ld_wk.wait()
    ld_wv.wait()
    sends = []

    def go(cp):
        cp.start()
        sends.append(cp)
        return cp

    to_r = [w_copy(i, own_w, slot(LEFT, 0), i, dev(RIGHT, 0)) for i in range(3)]
    to_l = [w_copy(3 + i, own_w, slot(RIGHT, 0), i, dev(LEFT, 0)) for i in range(3)]
    to_s = rcopy(wbuf.at[own_w], wbuf.at[slot(0, 1)], w_send.at[6], w_recv.at[slot(0, 1) * 4], dev(0, 1))
    for cp in (to_r[0], to_l[0], to_r[1], to_l[1], to_s):
        go(cp)
    fwd_r = w_copy(7, slot(LEFT, 0), slot(OPP, 0), 0, dev(RIGHT, 0))
    fwd_l = w_copy(8, slot(RIGHT, 0), slot(OPP, 0), 1, dev(LEFT, 0))
    to_p = {(rel, i): w_copy(9 + n, slot(rel, 0), slot(rel, 0), i, partner, 3 - i)
            for n, (rel, i) in enumerate(((LEFT, 0), (RIGHT, 0), (OPP, 0), (OPP, 1)))}
    sib_fwd = {(rel, i): w_copy(13 + 4 * n + i, slot(rel, 0), slot(rel, 1), i, dev(0, 1))
               for n, rel in enumerate((LEFT, RIGHT, OPP)) for i in range(4)}

    ld_wq = pltpu.make_async_copy(wq, wq_v, ldsem.at[2])
    ld_wg = pltpu.make_async_copy(wg, wg_v, ldsem.at[3])
    ld_wu = pltpu.make_async_copy(wu, wu_v, ldsem.at[4])

    gain = g_attn[...].astype(F32)
    pos0 = me * seq_loc

    @pl.loop(0, n_batch)
    def _(b):
        s = lax.rem(b, n_x)

        @pl.when(b + n_x - 1 < n_batch)
        def _():
            x_copy(b + n_x - 1, lax.rem(b + n_x - 1, n_x)).start()

        x_copy(b, s).wait()
        x = xbuf[s].astype(F32)
        normed[pl.ds(pl.multiple_of(b * seq_loc, seq_loc), seq_loc), :] = norm_rows(x, gain).astype(BF16)
        here = (lax.broadcasted_iota(jnp.int32, (seq_loc, 1), 0) + pos0 == lens[b] - 1).astype(F32)
        last_f[pl.ds(b, 1), :] = jnp.sum(x * here, axis=0, keepdims=True)
        len_v[pl.ds(b, 1), :] = jnp.full((1, HEAD_DIM), lens[b], jnp.int32)

    ld_wq.start()
    ld_wg.start()
    ld_wu.start()

    xl_own[...] = last_f[...].astype(BF16)
    xl_a = go(rcopy(xl_own, xl_sib, xl_send.at[0], xl_rsem.at[0], dev(0, 1)))

    def table(cos_ref, sin_ref, rows, pos):
        lane = lax.broadcasted_iota(jnp.int32, pos.shape, 1)
        hd = HEAD_DIM // 2
        step = jnp.where(lane < hd, lane, lane - hd).astype(F32)
        angle = pos.astype(F32) * jnp.exp(step * (-2.0 * math.log(10000.0) / HEAD_DIM))
        cos_ref[rows, :] = jnp.cos(angle)
        sin_ref[rows, :] = jnp.where(lane < hd, -1.0, 1.0) * jnp.sin(angle)

    table(cos_pos, sin_pos, pl.ds(0, seq_loc), lax.broadcasted_iota(jnp.int32, (seq_loc, HEAD_DIM), 0) + pos0)
    table(cos_row, sin_row, pl.ds(0, n_batch), len_v[...] - 1)
    table(cos_row, sin_row, pl.ds(n_batch, n_batch), len_v[...])

    hb = n_batch // CORES
    xl_a.wait_recv()
    my_rows = pl.ds(pl.multiple_of(k * hb, hb), hb)
    oth_rows = pl.ds(pl.multiple_of(o_core * hb, hb), hb)
    xl_sum[...] = xl_own[my_rows, :] + xl_sib[my_rows, :]
    xl_b = [go(rcopy(xl_sum, xl_recv.at[n_chip - 1 - rel], xl_send.at[rel], xl_rsem.at[n_chip - rel], dev(rel, 0))) for rel in (RIGHT, LEFT, OPP)]
    go(to_r[2])
    go(to_l[2])

    def head(sl, dst):
        for_rows = 512

        @pl.loop(0, n_tok // for_rows)
        def _(m):
            r0 = pl.multiple_of(m * for_rows, for_rows)
            res = dot_f32(normed[pl.ds(r0, for_rows), :], wbuf[sl])
            res_k[pl.ds(r0, for_rows), :] = res[:, :HEAD_DIM]
            res_v[pl.ds(r0, for_rows), :] = res[:, HEAD_DIM:]

        @pl.loop(0, seq_loc, unroll=4)
        def _(s):
            rows = pl.ds(pl.multiple_of(s * n_batch, n_batch), n_batch)
            kt = res_k[pl.ds(s, n_batch, stride=seq_loc), :]
            dst[0, rows, :] = rotate(kt, cos_pos[pl.ds(s, 1), :], sin_pos[pl.ds(s, 1), :]).astype(BF16)
            dst[1, rows, :] = res_v[pl.ds(s, n_batch, stride=seq_loc), :].astype(BF16)

    def kv_copy(n, rel, kk):
        sl = slot((n_chip - rel) % n_chip, kk)
        return rcopy(stage.at[slot(rel, kk) - 1], kvrecv.at[sl], kv_send.at[n], kv_recv.at[sl], dev(rel, kk))

    def wait_w(rel, kk, i):
        w_copy(0, slot(rel, kk), slot(rel, kk), i, dev(0, 1)).wait_recv()

    for rel in (LEFT, RIGHT):
        wait_w(rel, 0, 0)
        go(to_p[rel, 0])
        go(sib_fwd[rel, 0])
        if rel == LEFT:
            go(fwd_r)
    head(own_w, kvrecv.at[own_w])
    for rel in (RIGHT, LEFT):
        wait_w(rel, 0, 1)
        if rel == RIGHT:
            go(fwd_l)
        go(sib_fwd[rel, 1])
    to_s.wait_recv()
    head(slot(0, 1), stage.at[slot(0, 1) - 1])
    kv_sib = go(kv_copy(0, 0, 1))

    for cp in xl_b:
        cp.wait_recv()
    xl_half[...] = xl_sum[...] + xl_recv[0] + (xl_recv[1] + xl_recv[2])
    xl_c = go(rcopy(xl_half, xl_oth, xl_send.at[4], xl_rsem.at[4], dev(0, 1)))

    rows_f[my_rows, :] = xl_half[...].astype(F32)
    rows_f[pl.ds(n_batch, n_batch), :] = new_tok[...].astype(F32)
    ld_wq.wait()
    xl_c.wait_recv()
    rows_f[oth_rows, :] = xl_oth[...].astype(F32)
    rows_n[...] = norm_rows(rows_f[...], gain).astype(BF16)
    q_all = dot_f32(rows_n[...], wq_v[...])
    for g in range(heads_loc):
        q_g = rotate(q_all[:, g * HEAD_DIM:(g + 1) * HEAD_DIM], cos_row[...], sin_row[...])
        q_s[pl.ds(g * n_row, n_row), :] = q_g.astype(BF16)
    q_out = go(rcopy(q_s, q_in.at[0], pt_send.at[0], pt_recv.at[0], dev(OPP, 0)))
    q_fwd = rcopy(q_in.at[0], q_in.at[1], pt_send.at[1], pt_recv.at[1], dev(0, 1))
    kv_new = dot_f32(rows_n[...], wbuf[own_w])
    new_rows = slice(n_batch, n_row)
    k_new = rotate(kv_new[new_rows, :HEAD_DIM], cos_row[pl.ds(n_batch, n_batch), :], sin_row[pl.ds(n_batch, n_batch), :])
    kvnew[0] = k_new.astype(BF16)
    kvnew[1] = kv_new[new_rows, HEAD_DIM:].astype(BF16)

    for rel in (LEFT, RIGHT):
        for i in (3, 2):
            wait_w(rel, 0, i)
            go(sib_fwd[rel, i])
    n = 1
    kv_nb = {}
    for kk in range(2):
        for rel in (RIGHT, LEFT):
            if kk == 1:
                for i in range(4):
                    wait_w(rel, 1, i)
            head(slot(rel, kk), stage.at[slot(rel, kk) - 1])
            kv_nb[rel, kk] = go(kv_copy(n, rel, kk))
            n += 1
        if kk == 0:
            for i in range(2):
                wait_w(OPP, 0, i)
                go(to_p[OPP, i])
                go(sib_fwd[OPP, i])
    q_out.wait_recv()
    go(q_fwd)

    scale = HEAD_DIM ** -0.5
    n_q = heads_loc * n_row
    chunk = min(512, n_tok)
    mine = (m_s, l_s, acc_s)

    def reset(state):
        state[0][...] = jnp.full(state[0].shape, NEG_BIG, F32)
        state[1][...] = jnp.zeros(state[1].shape, F32)
        state[2][...] = jnp.zeros(state[2].shape, F32)

    def update(state, sc, valid, v_blk):
        m_r, l_r, acc_r = state
        sc = jnp.where(valid, sc * scale, NEG_BIG)
        m_old = m_r[...]
        m_new = jnp.maximum(m_old, jnp.max(sc, axis=-1, keepdims=True))
        prob = jnp.where(valid, jnp.exp(sc - m_new), 0.0)
        alpha = jnp.exp(m_old - m_new)
        l_r[...] = l_r[...] * alpha + jnp.sum(prob, axis=-1, keepdims=True)
        acc_r[...] = acc_r[...] * alpha + dot_f32(prob.astype(BF16), v_blk)
        m_r[...] = m_new

    def attend(state, q_ref, kv_ref, src):
        @pl.loop(0, n_tok // chunk)
        def _(ch):
            rows = pl.ds(pl.multiple_of(ch * chunk, chunk), chunk)
            sc = dot_bt(q_ref[...], kv_ref[0, rows, :])
            col = lax.broadcasted_iota(jnp.int32, (n_q, chunk), 1)
            row = lax.broadcasted_iota(jnp.int32, (n_q, chunk), 0)
            pos = src * seq_loc + ch * (chunk // n_batch) + col // n_batch
            len_row = jnp.concatenate([len_v[:, :1]] * (n_q // n_batch), axis=0)
            valid = (col % n_batch == row % n_batch) & (pos < len_row)
            update(state, sc, valid, kv_ref[1, rows, :])

    lane_rows = [(i, min(HEAD_DIM, n_q - i)) for i in range(0, n_q, HEAD_DIM)]

    def on_diag(size):
        return lax.broadcasted_iota(jnp.int32, (size, HEAD_DIM), 0) == lax.broadcasted_iota(jnp.int32, (size, HEAD_DIM), 1)

    def put_column(ref, r0, column):
        for j, (i, size) in enumerate(lane_rows):
            ref[pl.ds(r0 + j, 1), :] = jnp.sum(jnp.where(on_diag(size), column[i:i + size], 0.0), axis=0, keepdims=True)

    def get_column(ref, r0):
        cols = [jnp.sum(jnp.where(on_diag(size), ref[pl.ds(r0 + j, 1), :], 0.0), axis=1, keepdims=True) for j, (i, size) in enumerate(lane_rows)]
        return jnp.concatenate(cols, axis=0)

    reset(mine)
    col = lax.broadcasted_iota(jnp.int32, (n_q, n_batch), 1)
    row = lax.broadcasted_iota(jnp.int32, (n_q, n_batch), 0)
    is_new = (row // n_batch) % 2 == 1
    update(mine, dot_bt(q_s[...], kvnew[0]), (col == row % n_batch) & is_new, kvnew[1])
    attend(mine, q_s, kvrecv.at[own_w], me)
    kv_sib.wait_recv()
    attend(mine, q_s, kvrecv.at[slot(0, 1)], dev(0, 1))

    n_lr = len(lane_rows)
    other = (m_p, l_p, acc_p)

    def pack(state, ref):
        ref[pl.ds(0, n_q), :] = state[2][...]
        put_column(ref, n_q, state[0][...])
        put_column(ref, n_q + n_lr, state[1][...])

    def merge(state, ref):
        m_r, l_r, acc_r = state
        m_o, l_o = get_column(ref, n_q), get_column(ref, n_q + n_lr)
        m_old = m_r[...]
        m_new = jnp.maximum(m_old, m_o)
        f_mine, f_oth = jnp.exp(m_old - m_new), jnp.exp(m_o - m_new)
        l_r[...] = l_r[...] * f_mine + l_o * f_oth
        acc_r[...] = acc_r[...] * f_mine + ref[pl.ds(0, n_q), :] * f_oth
        m_r[...] = m_new

    for i in (3, 2):
        wait_w(OPP, 0, i)
        go(sib_fwd[OPP, i])
    for i in range(4):
        wait_w(OPP, 1, i)
    head(slot(OPP, 1), stage.at[slot(OPP, 1) - 1])
    q_fwd.wait_recv()
    reset(other)
    attend(other, q_in.at[1], stage.at[slot(OPP, 1) - 1], me)
    pack(other, msg.at[1])
    pt_sib = go(rcopy(msg.at[1], msg_in.at[1], pt_send.at[2], pt_recv.at[2], dev(0, 1)))
    head(slot(OPP, 0), stage.at[slot(OPP, 0) - 1])
    reset(other)
    attend(other, q_in.at[0], stage.at[slot(OPP, 0) - 1], me)
    pt_sib.wait_recv()
    merge(other, msg_in.at[1])
    pack(other, msg.at[0])
    pt_out = go(rcopy(msg.at[0], msg_in.at[0], pt_send.at[3], pt_recv.at[3], dev(OPP, 0)))

    per = n_tok // n_bulk
    bulk = []
    for kk in range(2):
        for i in range(2):
            for j in range(n_bulk):
                rows = pl.ds(j * per, per)
                x = len(bulk)
                bulk.append(rcopy(stage.at[slot(OPP, kk) - 1, i, rows, :], kvrecv.at[slot(OPP, kk), i, rows, :], bulk_send.at[x], bulk_recv.at[x], dev(OPP, kk)))
    waiting = list(bulk)

    def send_bulk(count):
        for _ in range(count):
            if waiting:
                go(waiting.pop(0))

    send_bulk(plan[0])

    wd_v = normed.at[pl.ds(0, ff_loc), :]
    wo_v = normed.at[pl.ds(ff_loc, heads_loc * HEAD_DIM), :]
    ld_wo = pltpu.make_async_copy(wo, wo_v, ldsem.at[0])
    ld_wd = pltpu.make_async_copy(wd, wd_v, ldsem.at[1])
    ld_wo.start()
    ld_wd.start()

    n = 2
    for kk in range(2):
        for rel in (RIGHT, LEFT):
            src_rel = (n_chip - rel) % n_chip
            kv_nb[rel, kk].wait_recv()
            attend(mine, q_s, kvrecv.at[slot(src_rel, kk)], dev(src_rel, kk))
            n += 1
    pt_out.wait_recv()
    merge(mine, msg_in.at[0])
    o_all = (acc_s[...] / l_s[...]).astype(BF16)

    def sum_over_model(i, part_r, d2d_r, sum_r, in_r):
        cp = go(rcopy(part_r.at[o_core], d2d_r, ar_send.at[4 * i], ar_recv.at[4 * i], dev(0, 1)))
        cp.wait_recv()
        cps = []
        for rel in (OPP, RIGHT, LEFT):
            chip = lax.rem(c + rel, n_chip)
            sum_r[rel] = part_r[k, chip] + d2d_r[chip]
            cps.append(go(rcopy(sum_r.at[rel], in_r.at[n_chip - 1 - rel], ar_send.at[4 * i + rel], ar_recv.at[4 * i + n_chip - rel], dev(rel, 0))))
        send_bulk(plan[1 + 2 * i])
        total = part_r[k, c] + d2d_r[c]
        for cp in cps[1:] + cps[:1]:
            cp.wait_recv()
        return total + in_r[0] + in_r[2] + in_r[1]

    def gather_rows(i, buf):
        cps = []
        for rel in (OPP, RIGHT, LEFT):
            cps.append(go(rcopy(buf.at[k, c], buf.at[k, c], ag_send.at[8 * i + rel], ag_recv.at[8 * i + n_chip - rel], dev(rel, 0))))
        cps.append(go(rcopy(buf.at[k, c], buf.at[k, c], ag_send.at[8 * i], ag_recv.at[8 * i], dev(0, 1))))
        send_bulk(plan[2 + 2 * i])
        fw = []
        for rel, cp in ((LEFT, cps[1]), (RIGHT, cps[2]), (OPP, cps[0])):
            cp.wait_recv()
            chip = lax.rem(c + rel, n_chip)
            fw.append(go(rcopy(buf.at[k, chip], buf.at[k, chip], ag_send.at[8 * i + 4 + rel], ag_recv.at[8 * i + 4 + rel], dev(0, 1))))
        for cp in [cps[3]] + fw:
            cp.wait_recv()

    ld_wo.wait()
    o_rows = jnp.concatenate([o_all[g * n_row:(g + 1) * n_row] for g in range(heads_loc)], axis=1)
    o_out = dot_f32(o_rows, wo_v[...])
    for p in range(n_dev):
        part[p // n_chip, p % n_chip] = o_out[p * piece:(p + 1) * piece]
    my_piece = pl.ds(pl.multiple_of((k * n_chip + c) * piece, piece), piece)
    att_sum = sum_over_model(0, part, d2d_in, rs_sum, rs_in)
    x1 = (rows_f[my_piece, :] + att_sum).astype(BF16).astype(F32)
    x1_f[...] = x1
    agbuf[k, c] = norm_rows(x1, g_mlp[...].astype(F32)).astype(BF16)
    gather_rows(0, agbuf)
    for p in range(0, n_dev, 2):
        two = [agbuf[i // n_chip, i % n_chip].astype(F32) for i in (p, p + 1)]
        hid_n[pl.ds(p * piece, 2 * piece), :] = jnp.concatenate(two, axis=0).astype(BF16)
    ld_wg.wait()
    ld_wu.wait()
    gate = dot_f32(hid_n[...], wg_v[...])
    up = dot_f32(hid_n[...], wu_v[...])
    mid = (gate * jax.nn.sigmoid(gate) * up).astype(BF16)
    ld_wd.wait()
    down = dot_f32(mid, wd_v[...])
    for p in range(n_dev):
        part2[p // n_chip, p % n_chip] = down[p * piece:(p + 1) * piece]
    mlp_sum = sum_over_model(1, part2, d2d_in2, rs_sum2, rs_in2)
    agbuf2[k, c] = (x1_f[...] + mlp_sum).astype(BF16)
    gather_rows(1, agbuf2)
    send_bulk(len(waiting))
    for p in range(0, n_dev, 2):
        two = jnp.concatenate([agbuf2[i // n_chip, i % n_chip].astype(F32) for i in (p, p + 1)], axis=0).astype(BF16)
        ref, r0 = (last_out, p * piece) if p * piece < n_batch else (dec_out, p * piece - n_batch)
        ref[pl.ds(r0, 2 * piece), :] = two
    for kk in range(2):
        for cp in bulk[kk * 2 * n_bulk:(kk + 1) * 2 * n_bulk]:
            cp.wait_recv()
        n += 1
    for cp in sends:
        cp.wait_send()


def write_kernel(n_dev, last_in, dec_in, kv, kv_new, last_out, dec_out, k_out, v_out, sem):
    n_tok = kv.shape[2]
    n_batch = kv_new.shape[1]
    me = lax.axis_index('model')
    pairs = [(last_in, last_out), (dec_in, dec_out)]
    for i, ref in enumerate((k_out, v_out)):
        pairs.append((kv_new.at[i], ref.at[pl.ds(n_dev * n_tok, n_batch), :]))
        for sl in range(n_dev):
            chip = lax.rem(me // CORES + sl // CORES, n_dev // CORES)
            core = lax.rem(me + sl, CORES)
            src = pl.ds(pl.multiple_of((CORES * chip + core) * n_tok, n_tok), n_tok)
            pairs.append((kv.at[sl, i], ref.at[src, :]))
    copies = [pltpu.make_async_copy(src, dst, sem.at[n]) for n, (src, dst) in enumerate(pairs)]
    for cp in copies:
        cp.start()
    for cp in copies:
        cp.wait()


def solution(mesh):
    n_dev = mesh.shape['model']
    assert n_dev == 4 * CORES and mesh.shape['replica'] % 2 == 0
    seq_spec = P('replica', 'model', None)
    col_spec = P(None, None, 'model')
    row_spec = P(None, 'model', None)
    gain_spec = P(None, None)
    tok_spec = P('replica', None)
    cache_spec = P(None, 'replica', None, 'model', None)
    in_specs = (seq_spec, P('replica'), tok_spec, gain_spec, col_spec, col_spec, col_spec, row_spec, gain_spec, col_spec, col_spec, row_spec)
    out_specs = (tok_spec, tok_spec, cache_spec, cache_spec)

    def per_device(prompt, lengths, new_tok, norm_attn, w_q, w_k, w_v, w_o, norm_mlp, w_gate, w_up, w_down):
        assert w_q.shape[0] == 1 and w_k.shape[2] == HEAD_DIM
        n_batch, seq_loc, d_model = prompt.shape
        n_tok = n_batch * seq_loc
        heads_loc = w_q.shape[2] // HEAD_DIM
        ff_loc = w_gate.shape[2]
        n_row = 2 * n_batch
        piece = n_row // n_dev
        n_chip = n_dev // CORES
        hb = n_batch // CORES
        n_q = heads_loc * n_row
        vm = pl.BlockSpec(memory_space=pltpu.VMEM)
        hbm = pl.BlockSpec(memory_space=pl.ANY)
        V = pltpu.VMEM
        DMA = pltpu.SemaphoreType.DMA
        slab = (2, n_tok, HEAD_DIM)
        wide = (CORES, n_chip, piece, d_model)
        n_lr = 2 * pl.cdiv(n_q, HEAD_DIM)
        state = [V((n_q, 1), F32), V((n_q, 1), F32), V((n_q, HEAD_DIM), F32)]
        note = V((2, pl.cdiv(n_q + n_lr, 8) * 8, HEAD_DIM), F32)
        scratch = [
            V((4, seq_loc, d_model), BF16), V((n_tok, d_model), BF16), V((n_dev, d_model, 2 * HEAD_DIM), BF16),
            V((n_dev - 1,) + slab, BF16),
            V((d_model, heads_loc * HEAD_DIM), BF16), V((d_model, ff_loc), BF16), V((d_model, ff_loc), BF16),
            V((n_tok, HEAD_DIM), F32), V((n_tok, HEAD_DIM), F32),
            V((n_batch, HEAD_DIM), jnp.int32), V((seq_loc, HEAD_DIM), F32), V((seq_loc, HEAD_DIM), F32), V((n_row, HEAD_DIM), F32), V((n_row, HEAD_DIM), F32),
            V((n_batch, d_model), F32), V((n_batch, d_model), BF16), V((n_batch, d_model), BF16), V((hb, d_model), BF16),
            V((n_chip - 1, hb, d_model), BF16), V((hb, d_model), BF16), V((hb, d_model), BF16),
            V((n_row, d_model), F32), V((n_row, d_model), BF16), V((n_q, HEAD_DIM), BF16), V((2, n_q, HEAD_DIM), BF16),
            *state, *state, note, note,
            V(wide, F32), V(wide[1:], F32), V(wide[1:], F32), V((n_chip - 1,) + wide[2:], F32), V(wide, BF16), V(wide[2:], F32),
            V((n_row, d_model), BF16),
            V(wide, F32), V(wide[1:], F32), V(wide[1:], F32), V((n_chip - 1,) + wide[2:], F32), V(wide, BF16),
            DMA((4,)), DMA((5,)), DMA((25,)), DMA((4 * n_dev,)), DMA((5,)), DMA((n_dev,)), DMA((4 * N_BULK,)), DMA((4 * N_BULK,)), DMA((4,)), DMA((4,)),
            DMA((5,)), DMA((5,)), DMA((8,)), DMA((8,)), DMA((16,)), DMA((16,)),
        ]
        cache_rows = (seq_loc * n_dev + 1) * n_batch
        cache = jax.ShapeDtypeStruct((cache_rows, HEAD_DIM), BF16)
        tok = jax.ShapeDtypeStruct((n_batch, d_model), BF16)
        made = pl.pallas_call(
            functools.partial(kernel, n_dev, n_batch, seq_loc, d_model, heads_loc, ff_loc, N_BULK, PLAN),
            out_shape=[V((n_batch, d_model), BF16), V((n_batch, d_model), BF16), V((n_dev,) + slab, BF16), V((2, n_batch, HEAD_DIM), BF16)],
            in_specs=[pl.BlockSpec(memory_space=pltpu.SMEM), hbm] + [vm] * 3 + [hbm] * 7,
            out_specs=[vm] * 4,
            scratch_shapes=scratch,
            compiler_params=pltpu.CompilerParams(collective_id=0, has_side_effects=True, vmem_limit_bytes=60_300_000),
        )(lengths, prompt, new_tok, norm_attn, norm_mlp, w_q[0], w_k[0], w_v[0], w_o[0], w_gate[0], w_up[0], w_down[0])
        last, dec, kc, vc = pl.pallas_call(
            functools.partial(write_kernel, n_dev),
            out_shape=[tok, tok, cache, cache],
            in_specs=[vm] * 4,
            out_specs=[hbm] * 4,
            scratch_shapes=[DMA((4 + 2 * n_dev,))],
            compiler_params=pltpu.CompilerParams(vmem_limit_bytes=1 << 20),
        )(*made)

        def as_cache(arr):
            return jnp.transpose(arr.reshape(1, seq_loc * n_dev + 1, 1, n_batch, HEAD_DIM), (0, 3, 1, 2, 4))

        return dec, last, as_cache(kc), as_cache(vc)

    return jax.shard_map(per_device, mesh=mesh, in_specs=in_specs, out_specs=out_specs, check_vma=False)
```

```python
import functools
import math

import jax
import jax.numpy as jnp
from jax import lax
from jax.experimental import pallas as pl
from jax.experimental.pallas import tpu as pltpu
from jax.sharding import PartitionSpec as P

HEAD_DIM = 128
NEG_BIG = -1e30
CORES = 2
N_BULK = 3
PLAN = (3, 2, 4, 2, 1)
MESH_ID = pl.DeviceIdType.MESH
BF16 = jnp.bfloat16
F32 = jnp.float32


def dot_f32(a, b):
    return jnp.dot(a, b, preferred_element_type=F32)


def dot_bt(a, b):
    return lax.dot_general(a, b, (((1,), (1,)), ((), ())), preferred_element_type=F32)


def norm_rows(x_f32, gain_f32):
    inv_rms = lax.rsqrt(jnp.mean(x_f32 * x_f32, axis=-1, keepdims=True) + 1e-5)
    return x_f32 * inv_rms * gain_f32


def rotate(x_f32, cos_full, sin_signed):
    return x_f32 * cos_full + pltpu.roll(x_f32, HEAD_DIM // 2, 1) * sin_signed


def kernel(n_dev, n_batch, seq_loc, d_model, heads_loc, ff_loc, n_bulk, plan,
           lens, prompt, new_tok, g_attn, g_mlp, wq, wk, wv, wo, wg, wu, wd,
           last_out, dec_out, kvrecv, kvnew,
           xbuf, normed, wbuf, stage, wq_v, wg_v, wu_v, res_k, res_v,
           len_v, cos_pos, sin_pos, cos_row, sin_row,
           last_f, xl_own, xl_sib, xl_sum, xl_recv, xl_half, xl_oth, rows_f, rows_n, q_s, q_in,
           m_s, l_s, acc_s, m_p, l_p, acc_p, msg, msg_in,
           part, d2d_in, rs_sum, rs_in, agbuf, x1_f, hid_n, part2, d2d_in2, rs_sum2, rs_in2, agbuf2,
           xsem, ldsem, w_send, w_recv, kv_send, kv_recv, bulk_send, bulk_recv, pt_send, pt_recv, xl_send, xl_rsem,
           ar_send, ar_recv, ag_send, ag_recv):
    n_chip = n_dev // CORES
    n_tok = n_batch * seq_loc
    n_row = 2 * n_batch
    piece = n_row // n_dev
    quarter = d_model // 4
    me = lax.axis_index('model')
    c = me // CORES
    k = me % CORES
    o_core = 1 - k
    replica = lax.axis_index('replica')
    odd = lax.rem(replica, 2)
    partner = {'replica': replica + 1 - 2 * odd}

    def dev(rel, kk):
        chip = lax.rem(c + rel, n_chip)
        return CORES * chip + (k if kk == 0 else o_core)

    RIGHT, OPP, LEFT = 1, 2, 3

    def slot(rel, kk):
        return rel * CORES + kk

    def rcopy(src, dst, ssem, rsem, target):
        target = target if isinstance(target, dict) else {'model': target}
        return pltpu.make_async_remote_copy(src_ref=src, dst_ref=dst, send_sem=ssem, recv_sem=rsem,
                                            device_id=target, device_id_type=MESH_ID)

    own_w = slot(0, 0)
    ld_wk = pltpu.make_async_copy(wk, wbuf.at[own_w, :, pl.ds(0, HEAD_DIM)], ldsem.at[0])
    ld_wv = pltpu.make_async_copy(wv, wbuf.at[own_w, :, pl.ds(HEAD_DIM, HEAD_DIM)], ldsem.at[1])
    ld_wk.start()
    ld_wv.start()
    n_x = xbuf.shape[0]

    def x_copy(b, s):
        return pltpu.make_async_copy(prompt.at[b], xbuf.at[s], xsem.at[s])

    for b in range(n_x - 1):
        x_copy(b, b).start()

    barrier = pltpu.get_barrier_semaphore()
    for d in range(1, n_dev):
        pl.semaphore_signal(barrier, inc=1, device_id={'model': lax.rem(me + d, n_dev)}, device_id_type=MESH_ID)
    pl.semaphore_signal(barrier, inc=1, device_id=partner, device_id_type=MESH_ID)
    pl.semaphore_wait(barrier, n_dev)

    order = [i + odd * (3 - 2 * i) for i in range(4)]

    def w_part(sl, i):
        return wbuf.at[sl, pl.ds(pl.multiple_of(order[i] * quarter, quarter), quarter), :]

    def w_copy(n, src_slot, dst_slot, i, target, i_there=None):
        sem = w_recv.at[dst_slot * 4 + (i if i_there is None else i_there)]
        return rcopy(w_part(src_slot, i), w_part(dst_slot, i), w_send.at[n], sem, target)

    ld_wk.wait()
    ld_wv.wait()
    sends = []

    def go(cp):
        cp.start()
        sends.append(cp)
        return cp

    to_r = [w_copy(i, own_w, slot(LEFT, 0), i, dev(RIGHT, 0)) for i in range(3)]
    to_l = [w_copy(3 + i, own_w, slot(RIGHT, 0), i, dev(LEFT, 0)) for i in range(3)]
    to_s = rcopy(wbuf.at[own_w], wbuf.at[slot(0, 1)], w_send.at[6], w_recv.at[slot(0, 1) * 4], dev(0, 1))
    for cp in (to_r[0], to_l[0], to_r[1], to_l[1], to_s):
        go(cp)
    fwd_r = w_copy(7, slot(LEFT, 0), slot(OPP, 0), 0, dev(RIGHT, 0))
    fwd_l = w_copy(8, slot(RIGHT, 0), slot(OPP, 0), 1, dev(LEFT, 0))
    to_p = {(rel, i): w_copy(9 + n, slot(rel, 0), slot(rel, 0), i, partner, 3 - i)
            for n, (rel, i) in enumerate(((LEFT, 0), (RIGHT, 0), (OPP, 0), (OPP, 1)))}
    sib_fwd = {(rel, i): w_copy(13 + 4 * n + i, slot(rel, 0), slot(rel, 1), i, dev(0, 1))
               for n, rel in enumerate((LEFT, RIGHT, OPP)) for i in range(4)}

    ld_wq = pltpu.make_async_copy(wq, wq_v, ldsem.at[2])
    ld_wg = pltpu.make_async_copy(wg, wg_v, ldsem.at[3])
    ld_wu = pltpu.make_async_copy(wu, wu_v, ldsem.at[4])

    gain = g_attn[...].astype(F32)
    pos0 = me * seq_loc

    @pl.loop(0, n_batch)
    def _(b):
        s = lax.rem(b, n_x)

        @pl.when(b + n_x - 1 < n_batch)
        def _():
            x_copy(b + n_x - 1, lax.rem(b + n_x - 1, n_x)).start()

        x_copy(b, s).wait()
        x = xbuf[s].astype(F32)
        normed[pl.ds(pl.multiple_of(b * seq_loc, seq_loc), seq_loc), :] = norm_rows(x, gain).astype(BF16)
        here = (lax.broadcasted_iota(jnp.int32, (seq_loc, 1), 0) + pos0 == lens[b] - 1).astype(F32)
        last_f[pl.ds(b, 1), :] = jnp.sum(x * here, axis=0, keepdims=True)
        len_v[pl.ds(b, 1), :] = jnp.full((1, HEAD_DIM), lens[b], jnp.int32)

    ld_wq.start()
    ld_wg.start()
    ld_wu.start()

    xl_own[...] = last_f[...].astype(BF16)
    xl_a = go(rcopy(xl_own, xl_sib, xl_send.at[0], xl_rsem.at[0], dev(0, 1)))

    def table(cos_ref, sin_ref, rows, pos):
        lane = lax.broadcasted_iota(jnp.int32, pos.shape, 1)
        hd = HEAD_DIM // 2
        step = jnp.where(lane < hd, lane, lane - hd).astype(F32)
        angle = pos.astype(F32) * jnp.exp(step * (-2.0 * math.log(10000.0) / HEAD_DIM))
        cos_ref[rows, :] = jnp.cos(angle)
        sin_ref[rows, :] = jnp.where(lane < hd, -1.0, 1.0) * jnp.sin(angle)

    table(cos_pos, sin_pos, pl.ds(0, seq_loc), lax.broadcasted_iota(jnp.int32, (seq_loc, HEAD_DIM), 0) + pos0)
    table(cos_row, sin_row, pl.ds(0, n_batch), len_v[...] - 1)
    table(cos_row, sin_row, pl.ds(n_batch, n_batch), len_v[...])

    hb = n_batch // CORES
    xl_a.wait_recv()
    my_rows = pl.ds(pl.multiple_of(k * hb, hb), hb)
    oth_rows = pl.ds(pl.multiple_of(o_core * hb, hb), hb)
    xl_sum[...] = xl_own[my_rows, :] + xl_sib[my_rows, :]
    xl_b = [go(rcopy(xl_sum, xl_recv.at[n_chip - 1 - rel], xl_send.at[rel], xl_rsem.at[n_chip - rel], dev(rel, 0))) for rel in (RIGHT, LEFT, OPP)]
    go(to_r[2])
    go(to_l[2])

    def head(sl, dst):
        for_rows = 512

        @pl.loop(0, n_tok // for_rows)
        def _(m):
            r0 = pl.multiple_of(m * for_rows, for_rows)
            res = dot_f32(normed[pl.ds(r0, for_rows), :], wbuf[sl])
            res_k[pl.ds(r0, for_rows), :] = res[:, :HEAD_DIM]
            res_v[pl.ds(r0, for_rows), :] = res[:, HEAD_DIM:]

        @pl.loop(0, seq_loc, unroll=4)
        def _(s):
            rows = pl.ds(pl.multiple_of(s * n_batch, n_batch), n_batch)
            kt = res_k[pl.ds(s, n_batch, stride=seq_loc), :]
            dst[0, rows, :] = rotate(kt, cos_pos[pl.ds(s, 1), :], sin_pos[pl.ds(s, 1), :]).astype(BF16)
            dst[1, rows, :] = res_v[pl.ds(s, n_batch, stride=seq_loc), :].astype(BF16)

    def kv_copy(n, rel, kk):
        sl = slot((n_chip - rel) % n_chip, kk)
        return rcopy(stage.at[slot(rel, kk) - 1], kvrecv.at[sl], kv_send.at[n], kv_recv.at[sl], dev(rel, kk))

    def wait_w(rel, kk, i):
        w_copy(0, slot(rel, kk), slot(rel, kk), i, dev(0, 1)).wait_recv()

    for rel in (LEFT, RIGHT):
        wait_w(rel, 0, 0)
        go(to_p[rel, 0])
        go(sib_fwd[rel, 0])
        if rel == LEFT:
            go(fwd_r)
    head(own_w, kvrecv.at[own_w])
    for rel in (RIGHT, LEFT):
        wait_w(rel, 0, 1)
        if rel == RIGHT:
            go(fwd_l)
        go(sib_fwd[rel, 1])
    to_s.wait_recv()
    head(slot(0, 1), stage.at[slot(0, 1) - 1])
    kv_sib = go(kv_copy(0, 0, 1))

    for cp in xl_b:
        cp.wait_recv()
    xl_half[...] = xl_sum[...] + xl_recv[0] + (xl_recv[1] + xl_recv[2])
    xl_c = go(rcopy(xl_half, xl_oth, xl_send.at[4], xl_rsem.at[4], dev(0, 1)))

    rows_f[my_rows, :] = xl_half[...].astype(F32)
    rows_f[pl.ds(n_batch, n_batch), :] = new_tok[...].astype(F32)
    ld_wq.wait()
    xl_c.wait_recv()
    rows_f[oth_rows, :] = xl_oth[...].astype(F32)
    rows_n[...] = norm_rows(rows_f[...], gain).astype(BF16)
    q_all = dot_f32(rows_n[...], wq_v[...])
    for g in range(heads_loc):
        q_g = rotate(q_all[:, g * HEAD_DIM:(g + 1) * HEAD_DIM], cos_row[...], sin_row[...])
        q_s[pl.ds(g * n_row, n_row), :] = q_g.astype(BF16)
    q_out = go(rcopy(q_s, q_in.at[0], pt_send.at[0], pt_recv.at[0], dev(OPP, 0)))
    q_fwd = rcopy(q_in.at[0], q_in.at[1], pt_send.at[1], pt_recv.at[1], dev(0, 1))
    kv_new = dot_f32(rows_n[...], wbuf[own_w])
    new_rows = slice(n_batch, n_row)
    k_new = rotate(kv_new[new_rows, :HEAD_DIM], cos_row[pl.ds(n_batch, n_batch), :], sin_row[pl.ds(n_batch, n_batch), :])
    kvnew[0] = k_new.astype(BF16)
    kvnew[1] = kv_new[new_rows, HEAD_DIM:].astype(BF16)

    for rel in (LEFT, RIGHT):
        for i in (3, 2):
            wait_w(rel, 0, i)
            go(sib_fwd[rel, i])
    n = 1
    kv_nb = {}
    for kk in range(2):
        for rel in (RIGHT, LEFT):
            if kk == 1:
                for i in range(4):
                    wait_w(rel, 1, i)
            head(slot(rel, kk), stage.at[slot(rel, kk) - 1])
            kv_nb[rel, kk] = go(kv_copy(n, rel, kk))
            n += 1
        if kk == 0:
            for i in range(2):
                wait_w(OPP, 0, i)
                go(to_p[OPP, i])
                go(sib_fwd[OPP, i])
    q_out.wait_recv()
    go(q_fwd)

    scale = HEAD_DIM ** -0.5
    n_q = heads_loc * n_row
    chunk = min(512, n_tok)
    mine = (m_s, l_s, acc_s)

    def reset(state):
        state[0][...] = jnp.full(state[0].shape, NEG_BIG, F32)
        state[1][...] = jnp.zeros(state[1].shape, F32)
        state[2][...] = jnp.zeros(state[2].shape, F32)

    def update(state, sc, valid, v_blk):
        m_r, l_r, acc_r = state
        sc = jnp.where(valid, sc * scale, NEG_BIG)
        m_old = m_r[...]
        m_new = jnp.maximum(m_old, jnp.max(sc, axis=-1, keepdims=True))
        prob = jnp.where(valid, jnp.exp(sc - m_new), 0.0)
        alpha = jnp.exp(m_old - m_new)
        l_r[...] = l_r[...] * alpha + jnp.sum(prob, axis=-1, keepdims=True)
        acc_r[...] = acc_r[...] * alpha + dot_f32(prob.astype(BF16), v_blk)
        m_r[...] = m_new

    def attend(state, q_ref, kv_ref, src):
        @pl.loop(0, n_tok // chunk)
        def _(ch):
            rows = pl.ds(pl.multiple_of(ch * chunk, chunk), chunk)
            sc = dot_bt(q_ref[...], kv_ref[0, rows, :])
            col = lax.broadcasted_iota(jnp.int32, (n_q, chunk), 1)
            row = lax.broadcasted_iota(jnp.int32, (n_q, chunk), 0)
            pos = src * seq_loc + ch * (chunk // n_batch) + col // n_batch
            len_row = jnp.concatenate([len_v[:, :1]] * (n_q // n_batch), axis=0)
            valid = (col % n_batch == row % n_batch) & (pos < len_row)
            update(state, sc, valid, kv_ref[1, rows, :])

    lane_rows = [(i, min(HEAD_DIM, n_q - i)) for i in range(0, n_q, HEAD_DIM)]

    def on_diag(size):
        return lax.broadcasted_iota(jnp.int32, (size, HEAD_DIM), 0) == lax.broadcasted_iota(jnp.int32, (size, HEAD_DIM), 1)

    def put_column(ref, r0, column):
        for j, (i, size) in enumerate(lane_rows):
            ref[pl.ds(r0 + j, 1), :] = jnp.sum(jnp.where(on_diag(size), column[i:i + size], 0.0), axis=0, keepdims=True)

    def get_column(ref, r0):
        cols = [jnp.sum(jnp.where(on_diag(size), ref[pl.ds(r0 + j, 1), :], 0.0), axis=1, keepdims=True) for j, (i, size) in enumerate(lane_rows)]
        return jnp.concatenate(cols, axis=0)

    reset(mine)
    col = lax.broadcasted_iota(jnp.int32, (n_q, n_batch), 1)
    row = lax.broadcasted_iota(jnp.int32, (n_q, n_batch), 0)
    is_new = (row // n_batch) % 2 == 1
    update(mine, dot_bt(q_s[...], kvnew[0]), (col == row % n_batch) & is_new, kvnew[1])
    attend(mine, q_s, kvrecv.at[own_w], me)
    kv_sib.wait_recv()
    attend(mine, q_s, kvrecv.at[slot(0, 1)], dev(0, 1))

    n_lr = len(lane_rows)
    other = (m_p, l_p, acc_p)

    def pack(state, ref):
        ref[pl.ds(0, n_q), :] = state[2][...]
        put_column(ref, n_q, state[0][...])
        put_column(ref, n_q + n_lr, state[1][...])

    def merge(state, ref):
        m_r, l_r, acc_r = state
        m_o, l_o = get_column(ref, n_q), get_column(ref, n_q + n_lr)
        m_old = m_r[...]
        m_new = jnp.maximum(m_old, m_o)
        f_mine, f_oth = jnp.exp(m_old - m_new), jnp.exp(m_o - m_new)
        l_r[...] = l_r[...] * f_mine + l_o * f_oth
        acc_r[...] = acc_r[...] * f_mine + ref[pl.ds(0, n_q), :] * f_oth
        m_r[...] = m_new

    for i in (3, 2):
        wait_w(OPP, 0, i)
        go(sib_fwd[OPP, i])
    for i in range(4):
        wait_w(OPP, 1, i)
    head(slot(OPP, 1), stage.at[slot(OPP, 1) - 1])
    q_fwd.wait_recv()
    reset(other)
    attend(other, q_in.at[1], stage.at[slot(OPP, 1) - 1], me)
    pack(other, msg.at[1])
    pt_sib = go(rcopy(msg.at[1], msg_in.at[1], pt_send.at[2], pt_recv.at[2], dev(0, 1)))
    head(slot(OPP, 0), stage.at[slot(OPP, 0) - 1])
    reset(other)
    attend(other, q_in.at[0], stage.at[slot(OPP, 0) - 1], me)
    pt_sib.wait_recv()
    merge(other, msg_in.at[1])
    pack(other, msg.at[0])
    pt_out = go(rcopy(msg.at[0], msg_in.at[0], pt_send.at[3], pt_recv.at[3], dev(OPP, 0)))

    per = n_tok // n_bulk
    bulk = []
    for kk in range(2):
        for i in range(2):
            for j in range(n_bulk):
                rows = pl.ds(j * per, per)
                x = len(bulk)
                bulk.append(rcopy(stage.at[slot(OPP, kk) - 1, i, rows, :], kvrecv.at[slot(OPP, kk), i, rows, :], bulk_send.at[x], bulk_recv.at[x], dev(OPP, kk)))
    waiting = list(bulk)

    def send_bulk(count):
        for _ in range(count):
            if waiting:
                go(waiting.pop(0))

    send_bulk(plan[0])

    wd_v = normed.at[pl.ds(0, ff_loc), :]
    wo_v = normed.at[pl.ds(ff_loc, heads_loc * HEAD_DIM), :]
    ld_wo = pltpu.make_async_copy(wo, wo_v, ldsem.at[0])
    ld_wd = pltpu.make_async_copy(wd, wd_v, ldsem.at[1])
    ld_wo.start()
    ld_wd.start()

    n = 2
    for kk in range(2):
        for rel in (RIGHT, LEFT):
            src_rel = (n_chip - rel) % n_chip
            kv_nb[rel, kk].wait_recv()
            attend(mine, q_s, kvrecv.at[slot(src_rel, kk)], dev(src_rel, kk))
            n += 1
    pt_out.wait_recv()
    merge(mine, msg_in.at[0])
    o_all = (acc_s[...] / l_s[...]).astype(BF16)

    def sum_over_model(i, part_r, d2d_r, sum_r, in_r):
        cp = go(rcopy(part_r.at[o_core], d2d_r, ar_send.at[4 * i], ar_recv.at[4 * i], dev(0, 1)))
        cp.wait_recv()
        cps = []
        for rel in (OPP, RIGHT, LEFT):
            chip = lax.rem(c + rel, n_chip)
            sum_r[rel] = part_r[k, chip] + d2d_r[chip]
            cps.append(go(rcopy(sum_r.at[rel], in_r.at[n_chip - 1 - rel], ar_send.at[4 * i + rel], ar_recv.at[4 * i + n_chip - rel], dev(rel, 0))))
        send_bulk(plan[1 + 2 * i])
        total = part_r[k, c] + d2d_r[c]
        for cp in cps[1:] + cps[:1]:
            cp.wait_recv()
        return total + in_r[0] + in_r[2] + in_r[1]

    def gather_rows(i, buf):
        cps = []
        for rel in (OPP, RIGHT, LEFT):
            cps.append(go(rcopy(buf.at[k, c], buf.at[k, c], ag_send.at[8 * i + rel], ag_recv.at[8 * i + n_chip - rel], dev(rel, 0))))
        cps.append(go(rcopy(buf.at[k, c], buf.at[k, c], ag_send.at[8 * i], ag_recv.at[8 * i], dev(0, 1))))
        send_bulk(plan[2 + 2 * i])
        fw = []
        for rel, cp in ((LEFT, cps[1]), (RIGHT, cps[2]), (OPP, cps[0])):
            cp.wait_recv()
            chip = lax.rem(c + rel, n_chip)
            fw.append(go(rcopy(buf.at[k, chip], buf.at[k, chip], ag_send.at[8 * i + 4 + rel], ag_recv.at[8 * i + 4 + rel], dev(0, 1))))
        for cp in [cps[3]] + fw:
            cp.wait_recv()

    ld_wo.wait()
    o_rows = jnp.concatenate([o_all[g * n_row:(g + 1) * n_row] for g in range(heads_loc)], axis=1)
    o_out = dot_f32(o_rows, wo_v[...])
    for p in range(n_dev):
        part[p // n_chip, p % n_chip] = o_out[p * piece:(p + 1) * piece]
    my_piece = pl.ds(pl.multiple_of((k * n_chip + c) * piece, piece), piece)
    att_sum = sum_over_model(0, part, d2d_in, rs_sum, rs_in)
    x1 = (rows_f[my_piece, :] + att_sum).astype(BF16).astype(F32)
    x1_f[...] = x1
    agbuf[k, c] = norm_rows(x1, g_mlp[...].astype(F32)).astype(BF16)
    gather_rows(0, agbuf)
    for p in range(0, n_dev, 2):
        two = [agbuf[i // n_chip, i % n_chip].astype(F32) for i in (p, p + 1)]
        hid_n[pl.ds(p * piece, 2 * piece), :] = jnp.concatenate(two, axis=0).astype(BF16)
    ld_wg.wait()
    ld_wu.wait()
    gate = dot_f32(hid_n[...], wg_v[...])
    up = dot_f32(hid_n[...], wu_v[...])
    mid = (gate * jax.nn.sigmoid(gate) * up).astype(BF16)
    ld_wd.wait()
    down = dot_f32(mid, wd_v[...])
    for p in range(n_dev):
        part2[p // n_chip, p % n_chip] = down[p * piece:(p + 1) * piece]
    mlp_sum = sum_over_model(1, part2, d2d_in2, rs_sum2, rs_in2)
    agbuf2[k, c] = (x1_f[...] + mlp_sum).astype(BF16)
    gather_rows(1, agbuf2)
    send_bulk(len(waiting))
    for p in range(0, n_dev, 2):
        two = jnp.concatenate([agbuf2[i // n_chip, i % n_chip].astype(F32) for i in (p, p + 1)], axis=0).astype(BF16)
        ref, r0 = (last_out, p * piece) if p * piece < n_batch else (dec_out, p * piece - n_batch)
        ref[pl.ds(r0, 2 * piece), :] = two
    for kk in range(2):
        for cp in bulk[kk * 2 * n_bulk:(kk + 1) * 2 * n_bulk]:
            cp.wait_recv()
        n += 1
    for cp in sends:
        cp.wait_send()


def write_kernel(n_dev, last_in, dec_in, kv, kv_new, last_out, dec_out, k_out, v_out, sem):
    n_tok = kv.shape[2]
    n_batch = kv_new.shape[1]
    me = lax.axis_index('model')
    pairs = [(last_in, last_out), (dec_in, dec_out)]
    for i, ref in enumerate((k_out, v_out)):
        pairs.append((kv_new.at[i], ref.at[pl.ds(n_dev * n_tok, n_batch), :]))
        for sl in range(n_dev):
            chip = lax.rem(me // CORES + sl // CORES, n_dev // CORES)
            core = lax.rem(me + sl, CORES)
            src = pl.ds(pl.multiple_of((CORES * chip + core) * n_tok, n_tok), n_tok)
            pairs.append((kv.at[sl, i], ref.at[src, :]))
    copies = [pltpu.make_async_copy(src, dst, sem.at[n]) for n, (src, dst) in enumerate(pairs)]
    for cp in copies:
        cp.start()
    for cp in copies:
        cp.wait()


def solution(mesh):
    n_dev = mesh.shape['model']
    assert n_dev == 4 * CORES and mesh.shape['replica'] % 2 == 0
    seq_spec = P('replica', 'model', None)
    col_spec = P(None, None, 'model')
    row_spec = P(None, 'model', None)
    gain_spec = P(None, None)
    tok_spec = P('replica', None)
    cache_spec = P(None, 'replica', None, 'model', None)
    in_specs = (seq_spec, P('replica'), tok_spec, gain_spec, col_spec, col_spec, col_spec, row_spec, gain_spec, col_spec, col_spec, row_spec)
    out_specs = (tok_spec, tok_spec, cache_spec, cache_spec)

    def per_device(prompt, lengths, new_tok, norm_attn, w_q, w_k, w_v, w_o, norm_mlp, w_gate, w_up, w_down):
        assert w_q.shape[0] == 1 and w_k.shape[2] == HEAD_DIM
        n_batch, seq_loc, d_model = prompt.shape
        n_tok = n_batch * seq_loc
        heads_loc = w_q.shape[2] // HEAD_DIM
        ff_loc = w_gate.shape[2]
        n_row = 2 * n_batch
        piece = n_row // n_dev
        n_chip = n_dev // CORES
        hb = n_batch // CORES
        n_q = heads_loc * n_row
        vm = pl.BlockSpec(memory_space=pltpu.VMEM)
        hbm = pl.BlockSpec(memory_space=pl.ANY)
        V = pltpu.VMEM
        DMA = pltpu.SemaphoreType.DMA
        slab = (2, n_tok, HEAD_DIM)
        wide = (CORES, n_chip, piece, d_model)
        n_lr = 2 * pl.cdiv(n_q, HEAD_DIM)
        state = [V((n_q, 1), F32), V((n_q, 1), F32), V((n_q, HEAD_DIM), F32)]
        note = V((2, pl.cdiv(n_q + n_lr, 8) * 8, HEAD_DIM), F32)
        scratch = [
            V((4, seq_loc, d_model), BF16), V((n_tok, d_model), BF16), V((n_dev, d_model, 2 * HEAD_DIM), BF16),
            V((n_dev - 1,) + slab, BF16),
            V((d_model, heads_loc * HEAD_DIM), BF16), V((d_model, ff_loc), BF16), V((d_model, ff_loc), BF16),
            V((n_tok, HEAD_DIM), F32), V((n_tok, HEAD_DIM), F32),
            V((n_batch, HEAD_DIM), jnp.int32), V((seq_loc, HEAD_DIM), F32), V((seq_loc, HEAD_DIM), F32), V((n_row, HEAD_DIM), F32), V((n_row, HEAD_DIM), F32),
            V((n_batch, d_model), F32), V((n_batch, d_model), BF16), V((n_batch, d_model), BF16), V((hb, d_model), BF16),
            V((n_chip - 1, hb, d_model), BF16), V((hb, d_model), BF16), V((hb, d_model), BF16),
            V((n_row, d_model), F32), V((n_row, d_model), BF16), V((n_q, HEAD_DIM), BF16), V((2, n_q, HEAD_DIM), BF16),
            *state, *state, note, note,
            V(wide, F32), V(wide[1:], F32), V(wide[1:], F32), V((n_chip - 1,) + wide[2:], F32), V(wide, BF16), V(wide[2:], F32),
            V((n_row, d_model), BF16),
            V(wide, F32), V(wide[1:], F32), V(wide[1:], F32), V((n_chip - 1,) + wide[2:], F32), V(wide, BF16),
            DMA((4,)), DMA((5,)), DMA((25,)), DMA((4 * n_dev,)), DMA((5,)), DMA((n_dev,)), DMA((4 * N_BULK,)), DMA((4 * N_BULK,)), DMA((4,)), DMA((4,)),
            DMA((5,)), DMA((5,)), DMA((8,)), DMA((8,)), DMA((16,)), DMA((16,)),
        ]
        cache_rows = (seq_loc * n_dev + 1) * n_batch
        cache = jax.ShapeDtypeStruct((cache_rows, HEAD_DIM), BF16)
        tok = jax.ShapeDtypeStruct((n_batch, d_model), BF16)
        made = pl.pallas_call(
            functools.partial(kernel, n_dev, n_batch, seq_loc, d_model, heads_loc, ff_loc, N_BULK, PLAN),
            out_shape=[V((n_batch, d_model), BF16), V((n_batch, d_model), BF16), V((n_dev,) + slab, BF16), V((2, n_batch, HEAD_DIM), BF16)],
            in_specs=[pl.BlockSpec(memory_space=pltpu.SMEM), hbm] + [vm] * 3 + [hbm] * 7,
            out_specs=[vm] * 4,
            scratch_shapes=scratch,
            compiler_params=pltpu.CompilerParams(collective_id=0, has_side_effects=True, vmem_limit_bytes=60_300_000),
        )(lengths, prompt, new_tok, norm_attn, norm_mlp, w_q[0], w_k[0], w_v[0], w_o[0], w_gate[0], w_up[0], w_down[0])
        last, dec, kc, vc = pl.pallas_call(
            functools.partial(write_kernel, n_dev),
            out_shape=[tok, tok, cache, cache],
            in_specs=[vm] * 4,
            out_specs=[hbm] * 4,
            scratch_shapes=[DMA((4 + 2 * n_dev,))],
            compiler_params=pltpu.CompilerParams(vmem_limit_bytes=1 << 20),
        )(*made)

        def as_cache(arr):
            return jnp.transpose(arr.reshape(1, seq_loc * n_dev + 1, 1, n_batch, HEAD_DIM), (0, 3, 1, 2, 4))

        return dec, last, as_cache(kc), as_cache(vc)

    return jax.shard_map(per_device, mesh=mesh, in_specs=in_specs, out_specs=out_specs, check_vma=False)
```
